256 devices in a mesh: groups: 2 (over y), shard: 16 (over z), head: 4 (over x), pair: 2 (over core).
Axes of the slice: x: 4, y: 2, z: 16, core: 2. Of those that a mesh axis runs over, the one named last changes fastest.
The devices are a block of a 4x16x16 slice.
Arguments:
- prompt_tokens: bfloat16 [2048, 8, 8192], P('shard', 'groups'), parts along dimension 1, may hold values from -48 to 48
- draft_tokens: bfloat16 [2, 8, 8192], P(None, 'groups', 'shard'), parts along dimension 1, may hold values from -48 to 48
- w_query: bfloat16 [8192, 4096], P('shard', ('head', 'pair')), may hold values from -0.0625 to 0.0625
- w_key: bfloat16 [8192, 1024], P('shard', ('head', 'pair')), may hold values from -0.0625 to 0.0625
- w_value: bfloat16 [8192, 1024], P('shard', ('head', 'pair')), may hold values from -0.0625 to 0.0625
- w_out: bfloat16 [4096, 8192], P(('head', 'pair'), 'shard'), may hold values from -0.09375 to 0.09375
- block_map: int32 [64], P('groups'), parts along dimension 0, may hold values from 0 to 31, each once
- prompt_len: int32 [8], P('groups'), parts along dimension 0, may hold values from 512 to 2048
- owner: int32 [8, 32], P(('head', 'pair'), 'groups'), parts along dimension 1, may hold values from 0 to 15, each once within a row
Outputs:
- prefill_out: bfloat16 [2048, 8, 4096], P('shard', 'groups', ('head', 'pair')), parts along dimension 1
- draft_attn: bfloat16 [2, 32, 8, 128], P(None, ('groups', 'shard'), ('head', 'pair')), parts along dimension 1
- decode_out: bfloat16 [2, 8, 8192], P(None, 'groups', ('shard', 'head', 'pair')), parts along dimension 1
The draws below stay inside these ranges and needn't reach their ends.
There are 2 independent parts, one for each index of `groups`. The reference program is written for one: setup_inputs(seed, part) draws one part's arguments, and reference() takes and returns one part's arrays. A program takes and returns all parts, laid end to end along the dimension named above; an argument that names none is the same for every part. Nothing has to cross between parts.
Inputs may be any that keep to these rules, and one draw needn't show every extreme that they name: `owner`: each row is a permutation of the 16 decode slots. `block_map`: a permutation of the 32 blocks.
All inputs are finite; a program needn't handle non-finite values.
Results may differ from the reference program's by a relative error of at most 0.025.
Values may be sent and summed in bfloat16 or wider, within the bound.
A program may use at most 128 MiB of HBM per device.

```python
import math
import jax
import jax.numpy as jnp
from jax import lax

D = 8192
KVH = 8
HEAD_DIM = 128
G = 4
BLK = 64
SEQS = 4
STEPS = 2
BLOCKS = 32
PROMPT = 2048
SLOTS = 16


def scaled_normal(key, shape):
    base = jax.random.truncated_normal(jax.random.fold_in(key, 11), -6.0, 6.0, shape, jnp.float32)
    return base.astype(jnp.bfloat16)


def draw_prompt_tokens(key, part):
    return scaled_normal(key, (PROMPT, SEQS, D))


def draw_draft_tokens(key, part):
    return scaled_normal(jax.random.fold_in(key, 5), (STEPS, SEQS, D))


def touch_ends(values, rng, low, largest):
    longest = values.shape.index(max(values.shape))
    spots = []
    for shift in (0, 1):
        where = [jax.random.randint(jax.random.fold_in(rng, axis), (), 0, length) for axis, length in enumerate(values.shape)]
        where[longest] = (where[longest] + shift) % values.shape[longest]
        spots.append(tuple(where))
    return values.at[spots[0]].set(low).at[spots[1]].set(largest)


def block_levels(key, dims, shards, low, top_value):
    loudness, own = 1.0, jax.random.fold_in(key, 6)
    for axis_at, blocks in shards:
        draws = jnp.exp(jax.random.uniform(jax.random.fold_in(own, axis_at), (blocks,), jnp.float32, low / len(shards), top_value / len(shards)))
        loudness = loudness * jnp.repeat(draws, dims[axis_at] // blocks).reshape([-1 if axis == axis_at else 1 for axis in range(len(dims))])
    return loudness


def scatter_about(stream_key, extent, spread, limit, shards=(), kind=jnp.bfloat16):
    drawn = jax.random.normal(stream_key, extent, jnp.float32) * spread
    if len(shards) > 0:
        drawn = block_levels(stream_key, extent, shards, -0.22, 0.18) * drawn
    return jnp.clip(drawn, min=-limit, max=limit).astype(kind)


def setup_inputs(seed: int = 0, part: int = 0) -> dict:
    seeds = jax.random.split(jax.random.key(seed), 10)
    part_splits = jax.random.split(jax.random.fold_in(seeds[9], part), 10)
    prompt_tokens = draw_prompt_tokens(jax.random.fold_in(jax.random.fold_in(seeds[9], part), 71), part)
    draft_tokens = draw_draft_tokens(jax.random.fold_in(jax.random.fold_in(seeds[9], part), 71), part)
    w_query = scatter_about(seeds[2], (D, KVH * G * HEAD_DIM), D ** -0.5, 0.0625, ((0, 16), (1, 8)))
    w_key = scatter_about(seeds[3], (D, KVH * HEAD_DIM), D ** -0.5, 0.0625, ((0, 16), (1, 8)))
    w_value = scatter_about(seeds[4], (D, KVH * HEAD_DIM), D ** -0.5, 0.0625, ((0, 16), (1, 8)))
    w_out = scatter_about(seeds[5], (KVH * G * HEAD_DIM, D), (KVH * G * HEAD_DIM) ** -0.5, 0.09375, ((0, 8), (1, 16)))
    block_map = jax.random.permutation(part_splits[6], BLOCKS).astype(jnp.int32)
    prompt_len = touch_ends(jax.random.randint(part_splits[7], (SEQS,), PROMPT // 4, PROMPT + 1), jax.random.fold_in(part_splits[7], 1), PROMPT // 4, PROMPT).astype(jnp.int32)
    owner = jax.vmap(lambda own: jax.random.permutation(own, SLOTS))(jax.random.split(part_splits[8], KVH)).reshape((KVH, SLOTS)).astype(jnp.int32)
    return {"prompt_tokens": prompt_tokens, "draft_tokens": draft_tokens, "w_query": w_query, "w_key": w_key, "w_value": w_value, "w_out": w_out, "block_map": block_map, "prompt_len": prompt_len, "owner": owner}


NEG = -1e+30
THETA = 500000.0

def rotate(vec, pos):
    half = vec.shape[-1] // 2
    freq = jnp.exp(jnp.arange(half, dtype=jnp.float32) * (-math.log(THETA) / half))
    angle = pos.astype(jnp.float32)[..., None] * freq
    cosine = jnp.cos(angle)
    sine = jnp.sin(angle)
    first = vec[..., :half]
    second = vec[..., half:]
    return jnp.concatenate([first * cosine - second * sine, second * cosine + first * sine], -1)

def rounded(weight):
    return lax.optimization_barrier(weight.astype(jnp.bfloat16)).astype(jnp.float32)

def reference(prompt_tokens, draft_tokens, w_query, w_key, w_value, w_out, block_map, prompt_len, owner):
    scale = 1.0 / math.sqrt(HEAD_DIM)
    slot_pos = (jnp.repeat(block_map, BLK) * BLK + jnp.tile(jnp.arange(BLK, dtype=jnp.int32), BLOCKS)).astype(jnp.int32)
    rows = prompt_tokens.reshape(PROMPT * SEQS, D)
    query = jnp.dot(rows, w_query, preferred_element_type=jnp.float32).reshape(PROMPT, SEQS, KVH, G, HEAD_DIM)
    key = jnp.dot(rows, w_key, preferred_element_type=jnp.float32).reshape(PROMPT, SEQS, KVH, HEAD_DIM)
    value = jnp.dot(rows, w_value, preferred_element_type=jnp.float32).reshape(PROMPT, SEQS, KVH, HEAD_DIM)
    query = rotate(query, slot_pos[:, None, None, None]).astype(jnp.bfloat16)
    key = rotate(key, slot_pos[:, None, None]).astype(jnp.bfloat16)
    value = value.astype(jnp.bfloat16)

    def prefill_one(items):
        q_seq, k_seq, v_seq, length = items
        scores = jnp.einsum('rhgd,nhd->rhgn', q_seq.astype(jnp.float32), k_seq.astype(jnp.float32)) * scale
        valid = (slot_pos[None, :] <= slot_pos[:, None]) & (slot_pos[None, :] < length)
        valid = valid[:, None, None, :]
        top = lax.optimization_barrier(jnp.max(jnp.where(valid, scores, NEG), -1, keepdims=True))
        weight = jnp.where(valid, jnp.exp(scores - top), 0.0)
        total = lax.optimization_barrier(jnp.sum(weight, -1))
        mixed = jnp.einsum('rhgn,nhd->rhgd', rounded(weight), v_seq.astype(jnp.float32))
        return (mixed / total[..., None]).astype(jnp.bfloat16)
    prefill = lax.map(prefill_one, (query.transpose(1, 0, 2, 3, 4), key.transpose(1, 0, 2, 3), value.transpose(1, 0, 2, 3), prompt_len))
    prefill_out = prefill.transpose(1, 0, 2, 3, 4).reshape(PROMPT, SEQS, KVH * G * HEAD_DIM)
    drafts = draft_tokens.reshape(STEPS * SEQS, D)
    draft_q = jnp.dot(drafts, w_query, preferred_element_type=jnp.float32).reshape(STEPS, SEQS, KVH, G, HEAD_DIM)
    draft_k = jnp.dot(drafts, w_key, preferred_element_type=jnp.float32).reshape(STEPS, SEQS, KVH, HEAD_DIM)
    draft_v = jnp.dot(drafts, w_value, preferred_element_type=jnp.float32).reshape(STEPS, SEQS, KVH, HEAD_DIM)
    draft_pos = (prompt_len[None, :] + jnp.arange(STEPS, dtype=jnp.int32)[:, None]).astype(jnp.int32)
    draft_q = rotate(draft_q, draft_pos[:, :, None, None]).astype(jnp.bfloat16)
    draft_k = rotate(draft_k, draft_pos[:, :, None]).astype(jnp.bfloat16)
    draft_v = draft_v.astype(jnp.bfloat16)
    old = jnp.einsum('tshgd,pshd->shtgp', draft_q.astype(jnp.float32), key.astype(jnp.float32)) * scale
    old_valid = (slot_pos[None, :] < prompt_len[:, None])[:, None, None, None, :]
    new = jnp.einsum('tshgd,ushd->shtgu', draft_q.astype(jnp.float32), draft_k.astype(jnp.float32)) * scale
    steps_row = jnp.arange(STEPS, dtype=jnp.int32)
    new_valid = (steps_row[None, :] <= steps_row[:, None])[None, None, :, None, :]
    top = jnp.maximum(lax.optimization_barrier(jnp.max(jnp.where(old_valid, old, NEG), -1)), lax.optimization_barrier(jnp.max(jnp.where(new_valid, new, NEG), -1)))[..., None]
    w_old = jnp.where(old_valid, jnp.exp(old - top), 0.0)
    w_new = jnp.where(new_valid, jnp.exp(new - top), 0.0)
    total = lax.optimization_barrier(jnp.sum(w_old, -1)) + lax.optimization_barrier(jnp.sum(w_new, -1))
    mixed = jnp.einsum('shtgp,pshd->shtgd', rounded(w_old), value.astype(jnp.float32))
    mixed = mixed + jnp.einsum('shtgu,ushd->shtgd', rounded(w_new), draft_v.astype(jnp.float32))
    attn = (mixed / total[..., None]).astype(jnp.bfloat16)
    slot_ids = jnp.arange(SLOTS, dtype=jnp.int32)
    match = owner[:, :, None] == slot_ids[None, None, :]
    inverse = lax.optimization_barrier(jnp.sum(jnp.where(match, slot_ids[None, :, None], 0), axis=1)).astype(jnp.int32)
    by_pair = attn.transpose(1, 0, 3, 2, 4).reshape(KVH, SEQS * G, STEPS, HEAD_DIM)
    taken = jnp.take_along_axis(by_pair, inverse[:, :, None, None], axis=1)
    draft_attn = taken.transpose(2, 1, 0, 3)
    by_seq = attn.transpose(2, 0, 1, 3, 4).reshape(STEPS * SEQS, KVH * G * HEAD_DIM)
    decode_out = jnp.dot(by_seq, w_out, preferred_element_type=jnp.float32).astype(jnp.bfloat16).reshape(STEPS, SEQS, D)
    return (prefill_out, draft_attn, decode_out)
```

```python
import functools
import math

import jax
import jax.numpy as jnp
from jax import lax
from jax.experimental import pallas as pl
from jax.experimental.pallas import tpu as pltpu
from jax.sharding import PartitionSpec as P

HEAD_DIM = 128
G = 4
BLK = 64
NEG = -1e30
THETA = 500000.0
MESH = pl.DeviceIdType.MESH
F32 = jnp.float32
BF16 = jnp.bfloat16
FAR = 1 << 30


def rope_tables(pos):
    lane = lax.broadcasted_iota(jnp.int32, (pos.shape[0], HEAD_DIM), 1)
    half = HEAD_DIM // 2
    pair = jnp.where(lane < half, lane, lane - half).astype(F32)
    freq = jnp.exp(pair * (-math.log(THETA) / half))
    angle = pos.astype(F32) * freq
    sine = jnp.sin(angle)
    return jnp.cos(angle), jnp.where(lane < half, -sine, sine)


def rope(v, cosine, sine):
    return v * cosine + pltpu.roll(v, HEAD_DIM // 2, 1) * sine


def kernel(
    shards, heads, pairs,
    x_hbm, d_ref, wq_hbm, wk_hbm, wv_hbm, wo_hbm, map_ref, len_ref, owner_ref,
    out_hbm, dattn_ref, dec_ref,
    buf, xin, xs, dbuf, acc, qbuf, sbuf, pbuf, lbuf, obuf, ostage, oready, cosb, sinb, dcos, dsin, kpos,
    dkv, aflat, lhs, wo, part, parts,
    load_sem, x_sem, out_sem, send_sem, recv_sem, dsend_sem, drecv_sem, psend_sem, precv_sem,
):
    me = lax.axis_index("shard")
    head = lax.axis_index("head")
    pair = lax.axis_index("pair")
    right = lax.rem(me + 1, shards)
    left = lax.rem(me + shards - 1, shards)
    far = shards // 2
    rows, seqs, width = x_hbm.shape
    depth = wq_hbm.shape[0]
    steps = d_ref.shape[0]
    tall = rows * seqs
    drafts = steps * seqs
    keys = shards * rows
    per = rows // BLK
    scale = 1.0 / math.sqrt(HEAD_DIM)
    peers = heads * pairs
    place = head * pairs + pair

    barrier = pltpu.get_barrier_semaphore()
    for z in (left, right):
        pl.semaphore_signal(barrier, inc=1, device_id={"shard": z}, device_id_type=MESH)
    for k in range(1, peers):
        other = lax.rem(place + k, peers)
        pl.semaphore_signal(
            barrier, inc=1, device_id={"head": other // pairs, "pair": other % pairs}, device_id_type=MESH
        )

    sources = {0: wk_hbm, 1: wv_hbm, 2: wq_hbm.at[:, 0:128], 3: wq_hbm.at[:, 128:256],
               6: wq_hbm.at[:, 256:384], 7: wq_hbm.at[:, 384:512]}
    loads = {s: pltpu.make_async_copy(src, buf.at[s, me], load_sem.at[s]) for s, src in sources.items()}
    wo_load = pltpu.make_async_copy(wo_hbm, wo, load_sem.at[4])
    for s in loads:
        loads[s].start()

    def x_load(owner):
        return pltpu.make_async_copy(
            x_hbm.at[:, :, pl.ds(pl.multiple_of(owner * depth, depth), depth)], xin.at[owner], x_sem.at[owner]
        )

    x_load(me).start()

    def start_x(s, _):
        x_load(lax.rem(me + shards - s, shards)).start()

        @pl.when(s < far)
        def _():
            x_load(lax.rem(me + s, shards)).start()

        return 0

    lax.fori_loop(1, far + 1, start_x, 0)
    wo_load.start()

    d_all = d_ref[...].astype(F32)
    dbuf[me] = jnp.concatenate([d_all[t] for t in range(steps)], 0).astype(BF16)

    pl.semaphore_wait(barrier, 2 + peers - 1)

    def hop(stream, way, s):
        owner = lax.rem(me + shards - (s - 1), shards) if way == 0 else lax.rem(me + (s - 1), shards)
        half = depth // 2
        if isinstance(s, int) and s == far:
            ref = buf.at[stream, owner, pl.ds(way * half, half)]
        else:
            ref = buf.at[stream, owner]
        return pltpu.make_async_remote_copy(
            src_ref=ref, dst_ref=ref, send_sem=send_sem.at[stream, way, s - 1], recv_sem=recv_sem.at[stream, way, s - 1],
            device_id={"shard": right if way == 0 else left}, device_id_type=MESH,
        )

    def draft_hop(way, s):
        owner = lax.rem(me + shards - (s - 1), shards) if way == 0 else lax.rem(me + (s - 1), shards)
        return pltpu.make_async_remote_copy(
            src_ref=dbuf.at[owner], dst_ref=dbuf.at[owner], send_sem=dsend_sem.at[way, s - 1],
            recv_sem=drecv_sem.at[way, s - 1], device_id={"shard": right if way == 0 else left}, device_id_type=MESH,
        )

    def launch(phase, s):
        for k in range(2):
            for way in range(2):
                hop(2 * phase + k, way, s).start()

    def arrive(phase, s):
        for k in range(2):
            for way in range(2):
                hop(2 * phase + k, way, s).wait_recv()

    slot_of = {0: 0, 1: 1, 3: 2}

    def multiply(phase, owner, first=False):
        w = jnp.concatenate([buf[2 * phase, owner], buf[2 * phase + 1, owner]], 1)
        got = jnp.dot(xs[owner], w, preferred_element_type=F32)
        for k in range(2):
            slot = 2 * slot_of[phase] + k
            if first:
                acc[slot] = got[:, k * HEAD_DIM : (k + 1) * HEAD_DIM]
            else:
                acc[slot] += got[:, k * HEAD_DIM : (k + 1) * HEAD_DIM]

    def fetch_rows(owner):
        x_load(owner).wait()
        xs[owner, 0:tall] = xin[owner].reshape(tall, depth)
        xs[owner, tall : tall + drafts] = dbuf[owner]

    def ring(phase, local, work, ready_next):
        def step(s, _):
            arrive(phase, s)
            if phase == 0:
                draft_hop(0, s).wait_recv()
                draft_hop(1, s).wait_recv()
            if_last = s == far - 1

            @pl.when(jnp.logical_not(if_last))
            def _():
                launch(phase, s + 1)

            @pl.when(if_last)
            def _():
                launch(phase, far)

            if phase == 0:
                draft_hop(0, s + 1).start()

                @pl.when(jnp.logical_not(if_last))
                def _():
                    draft_hop(1, s + 1).start()

            work(s)
            return 0

        local()
        lax.fori_loop(1, far, step, 0)
        ready_next()
        arrive(phase, far)
        if phase == 0:
            draft_hop(0, far).wait_recv()

    def both(phase):
        def work(s):
            def one(way, _):
                owner = lax.rem(me + shards + (2 * way - 1) * s, shards)
                if phase == 0:
                    fetch_rows(owner)
                multiply(phase, owner)
                return 0

            lax.fori_loop(0, 2, one, 0)

        return work

    opposite = lax.rem(me + far, shards)

    loads[0].wait()
    loads[1].wait()
    launch(0, 1)
    draft_hop(0, 1).start()
    draft_hop(1, 1).start()

    def local0():
        row = lax.broadcasted_iota(jnp.int32, (rows, 1), 0)
        pos = row + map_ref[me * per] * BLK
        for j in range(1, per):
            pos = jnp.where(row >= j * BLK, row - j * BLK + map_ref[me * per + j] * BLK, pos)
        cosb[...], sinb[...] = rope_tables(pos)
        drow = lax.broadcasted_iota(jnp.int32, (drafts, 1), 0)
        dpos = jnp.zeros((drafts, 1), jnp.int32)
        for t in range(steps):
            for b in range(seqs):
                dpos = jnp.where(drow == t * seqs + b, len_ref[b] + t, dpos)
        dcos[...], dsin[...] = rope_tables(dpos)
        for z in range(shards):
            lane = lax.broadcasted_iota(jnp.int32, (seqs, rows), 1)
            where = lane + map_ref[z * per] * BLK
            for j in range(1, per):
                where = jnp.where(lane >= j * BLK, lane - j * BLK + map_ref[z * per + j] * BLK, where)
            lengths = jnp.zeros((seqs, rows), jnp.int32)
            seq = lax.broadcasted_iota(jnp.int32, (seqs, rows), 0)
            for b in range(seqs):
                lengths = jnp.where(seq == b, len_ref[b], lengths)
            kpos[:, z * rows : (z + 1) * rows] = jnp.where(where < lengths, where, FAR)
        fetch_rows(me)
        multiply(0, me, True)

    def next0():
        loads[2].wait()
        loads[3].wait()
        launch(1, 1)

    ring(0, local0, both(0), next0)
    fetch_rows(opposite)
    multiply(0, opposite)

    def own_cache(b, _):
        k = acc[0, pl.ds(b, rows, stride=seqs), :]
        v = acc[1, pl.ds(b, rows, stride=seqs), :]
        at = pl.ds(pl.multiple_of(b * rows, rows), rows)
        buf[4, me, at] = rope(k, cosb[...], sinb[...]).astype(BF16)
        buf[5, me, at] = v.astype(BF16)
        return 0

    lax.fori_loop(0, seqs, own_cache, 0)
    dkv[0] = rope(acc[0, tall : tall + drafts, :], dcos[...], dsin[...]).astype(BF16)
    dkv[1] = acc[1, tall : tall + drafts, :].astype(BF16)

    ring(1, lambda: multiply(1, me, True), both(1), lambda: launch(2, 1))
    multiply(1, opposite)

    def queries(part):
        for b in range(seqs):
            for k in range(2):
                q = acc[2 + 2 * part + k, pl.ds(b, rows, stride=seqs), :]
                qbuf[b, k * rows : (k + 1) * rows] = rope(q, cosb[...], sinb[...]).astype(BF16)
        pieces = []
        dq = [rope(acc[2 + 2 * part + k, tall : tall + drafts, :], dcos[...], dsin[...])
              for k in range(2)]
        for b in range(seqs):
            pieces = [dq[k][t * seqs + b : t * seqs + b + 1] for k in range(2) for t in range(steps)]
            block = jnp.concatenate(pieces + [jnp.zeros((16 - 2 * steps, HEAD_DIM), F32)], 0)
            qbuf[b, 2 * rows : 2 * rows + 16] = block.astype(BF16)

    high = 2 * rows + 16

    def attend(part, b):
        cache_k = buf[4, :, pl.ds(pl.multiple_of(b * rows, rows), rows), :].reshape(keys, HEAD_DIM)
        cache_v = buf[5, :, pl.ds(pl.multiple_of(b * rows, rows), rows), :].reshape(keys, HEAD_DIM)
        q = qbuf[b]
        sbuf[...] = lax.dot_general(q, cache_k, (((1,), (1,)), ((), ())), preferred_element_type=F32)
        q_d = qbuf[b, 2 * rows : high]
        new = lax.dot_general(q_d, dkv[0], (((1,), (1,)), ((), ())), preferred_element_type=F32)
        r = lax.broadcasted_iota(jnp.int32, (16, drafts), 0)
        c = lax.broadcasted_iota(jnp.int32, (16, drafts), 1)
        seen = (lax.rem(c, seqs) == b) & (c // seqs <= lax.rem(r, steps))
        new = jnp.where(seen, new, NEG)
        new_top = jnp.max(new, 1, keepdims=True)
        kp = kpos[pl.ds(b, 1), :]

        def block(at, limit, floor):
            s = sbuf[pl.ds(at, 16), :]
            s = jnp.where(kp <= limit, s, NEG)
            top = jnp.max(s, 1, keepdims=True)
            if floor is not None:
                top = jnp.maximum(top, floor)
            w = jnp.exp((s - top) * scale)
            pbuf[pl.ds(at, 16), :] = w.astype(BF16)
            return top, jnp.sum(w, 1, keepdims=True)

        def prompt_block(i, _):
            at = pl.multiple_of(i * 16, 16)
            row = lax.rem(lax.broadcasted_iota(jnp.int32, (16, 1), 0) + at, rows)
            pos = row + map_ref[me * per] * BLK
            for j in range(1, per):
                pos = jnp.where(row >= j * BLK, row - j * BLK + map_ref[me * per + j] * BLK, pos)
            _, total = block(at, pos, None)
            lbuf[pl.ds(at, 16), :] = jnp.broadcast_to(total, (16, HEAD_DIM))
            return 0

        lax.fori_loop(0, 2 * rows // 16, prompt_block, 0, unroll=4)
        top, total = block(2 * rows, FAR - 1, new_top)
        w_new = jnp.where(seen, jnp.exp((new - top) * scale), 0.0)
        total = total + jnp.sum(w_new, 1, keepdims=True)
        obuf[...] = jnp.dot(pbuf[...], cache_v, preferred_element_type=F32)
        mixed = obuf[2 * rows : high] + jnp.dot(w_new.astype(BF16), dkv[1], preferred_element_type=F32)
        attn = (mixed / total).astype(BF16).astype(F32)
        aflat[pl.ds(pl.multiple_of(b * 2 * G, 2 * G) + part * 2 * steps, 2 * steps), :] = attn[0 : 2 * steps]
        for k in range(2):
            got = obuf[k * rows : (k + 1) * rows] / lbuf[k * rows : (k + 1) * rows]
            ostage[k, pl.ds(b, rows, stride=seqs), :] = got

    def put_out(part):
        for k in range(2):
            oready[:, :, (2 * part + k) * HEAD_DIM : (2 * part + k + 1) * HEAD_DIM] = (
                ostage[k].astype(BF16).reshape(rows, seqs, HEAD_DIM)
            )

    def next2():
        loads[6].wait()
        loads[7].wait()
        launch(3, 1)

    ring(2, lambda: queries(0), lambda s: None, next2)

    def work3(s):
        both(3)(s)

        @pl.when(s <= seqs)
        def _():
            attend(0, s - 1)

    ring(3, lambda: multiply(3, me, True), work3, lambda: put_out(0))
    multiply(3, opposite)
    queries(1)

    def last(b, _):
        attend(1, b)
        return 0

    lax.fori_loop(0, seqs, last, 0)

    wo_load.wait()
    for g in range(G):
        for t in range(steps):
            lhs[t * seqs : (t + 1) * seqs, g * HEAD_DIM : (g + 1) * HEAD_DIM] = aflat[
                pl.ds(g * steps + t, seqs, stride=G * steps), :
            ]
    partial = jnp.dot(lhs[...].astype(BF16), wo[...], preferred_element_type=F32)
    wide = partial.shape[1] // heads
    for h in range(heads):
        part[h] = partial[:, h * wide : (h + 1) * wide]
    parts[place] = part[head]

    def give(k):
        other = lax.rem(place + k, peers)
        return pltpu.make_async_remote_copy(
            src_ref=part.at[other // pairs], dst_ref=parts.at[place], send_sem=psend_sem.at[k], recv_sem=precv_sem.at[k],
            device_id={"head": other // pairs, "pair": other % pairs}, device_id_type=MESH,
        )

    for k in range(1, peers):
        give(k).start()
    put_out(1)
    store = pltpu.make_async_copy(oready, out_hbm, out_sem.at[0])
    store.start()

    r = lax.broadcasted_iota(jnp.int32, (seqs * G * steps, 1), 0)
    mine = jnp.zeros((seqs * G * steps, 1), jnp.int32)
    for p in range(seqs * G):
        mine = jnp.where(r // steps == p, owner_ref[0, p], mine)
    picked = jnp.where(mine == me, aflat[...], 0.0)
    for t in range(steps):
        dattn_ref[t, 0] = jnp.sum(
            jnp.where(lax.rem(r, steps) == t, picked, 0.0), 0, keepdims=True
        ).astype(BF16)

    for k in range(1, peers):
        give(k).wait_recv()
    summed = jnp.sum(parts[...], 0)
    narrow = wide // pairs
    got = summed[:, 0:narrow]
    for j in range(1, pairs):
        got = jnp.where(pair == j, summed[:, j * narrow : (j + 1) * narrow], got)
    for t in range(steps):
        dec_ref[t] = got[t * seqs : (t + 1) * seqs].astype(BF16)

    for k in range(1, peers):
        give(k).wait_send()

    def drain(s, _):
        for stream in range(8):
            for way in range(2):
                hop(stream, way, s).wait_send()
        for way in range(2):
            draft_hop(way, s).wait_send()
        return 0

    lax.fori_loop(1, far, drain, 0)
    for stream in range(8):
        for way in range(2):
            hop(stream, way, far).wait_send()
    draft_hop(0, far).wait_send()
    store.wait()


def body(shards, heads, pairs, x, d, wq, wk, wv, wo, block_map, prompt_len, owner):
    rows, seqs, width = x.shape
    depth = wq.shape[0]
    steps = d.shape[0]
    drafts = steps * seqs
    tall = rows * seqs
    keys = shards * rows
    peers = heads * pairs
    high = 2 * rows + 16
    any_ = pl.BlockSpec(memory_space=pl.ANY)
    vmem = pl.BlockSpec(memory_space=pltpu.VMEM)
    smem = pl.BlockSpec(memory_space=pltpu.SMEM)
    dma = pltpu.SemaphoreType.DMA
    return pl.pallas_call(
        functools.partial(kernel, shards, heads, pairs),
        out_shape=(
            jax.ShapeDtypeStruct((rows, seqs, wq.shape[1]), BF16),
            jax.ShapeDtypeStruct((steps, 1, 1, HEAD_DIM), BF16),
            jax.ShapeDtypeStruct((steps, seqs, wo.shape[1] // peers), BF16),
        ),
        in_specs=[any_, vmem, any_, any_, any_, any_, smem, smem, smem],
        out_specs=(any_, vmem, vmem),
        scratch_shapes=[
            pltpu.VMEM((8, shards, depth, HEAD_DIM), BF16),
            pltpu.VMEM((shards, rows, seqs, depth), BF16),
            pltpu.VMEM((shards, tall + drafts, depth), BF16),
            pltpu.VMEM((shards, drafts, depth), BF16),
            pltpu.VMEM((6, tall + drafts, HEAD_DIM), F32),
            pltpu.VMEM((seqs, high, HEAD_DIM), BF16),
            pltpu.VMEM((high, keys), F32),
            pltpu.VMEM((high, keys), BF16),
            pltpu.VMEM((2 * rows, HEAD_DIM), F32),
            pltpu.VMEM((high, HEAD_DIM), F32),
            pltpu.VMEM((2, tall, HEAD_DIM), F32),
            pltpu.VMEM((rows, seqs, wq.shape[1]), BF16),
            pltpu.VMEM((rows, HEAD_DIM), F32),
            pltpu.VMEM((rows, HEAD_DIM), F32),
            pltpu.VMEM((drafts, HEAD_DIM), F32),
            pltpu.VMEM((drafts, HEAD_DIM), F32),
            pltpu.VMEM((seqs, keys), jnp.int32),
            pltpu.VMEM((2, drafts, HEAD_DIM), BF16),
            pltpu.VMEM((seqs * G * steps, HEAD_DIM), F32),
            pltpu.VMEM((drafts, wq.shape[1]), F32),
            pltpu.VMEM(wo.shape, BF16),
            pltpu.VMEM((heads, drafts, wo.shape[1] // heads), F32),
            pltpu.VMEM((peers, drafts, wo.shape[1] // heads), F32),
            dma((8,)),
            dma((shards,)),
            dma((1,)),
            dma((8, 2, shards // 2)),
            dma((8, 2, shards // 2)),
            dma((2, shards // 2)),
            dma((2, shards // 2)),
            dma((peers,)),
            dma((peers,)),
        ],
        compiler_params=pltpu.CompilerParams(
            collective_id=0, has_side_effects=True, vmem_limit_bytes=60 * 1024 * 1024
        ),
    )(x, d, wq, wk, wv, wo, block_map, prompt_len, owner)


def solution(mesh):
    placed = (
        P("shard", "groups", None),
        P(None, "groups", "shard"),
        P("shard", ("head", "pair")),
        P("shard", ("head", "pair")),
        P("shard", ("head", "pair")),
        P(("head", "pair"), "shard"),
        P("groups"),
        P("groups"),
        P(("head", "pair"), "groups"),
    )
    return jax.shard_map(
        functools.partial(body, mesh.shape["shard"], mesh.shape["head"], mesh.shape["pair"]),
        mesh=mesh,
        in_specs=placed,
        out_specs=(
            P("shard", "groups", ("head", "pair")),
            P(None, ("groups", "shard"), ("head", "pair"), None),
            P(None, "groups", ("shard", "head", "pair")),
        ),
        check_vma=False,
    )
```

```python
import functools
import math

import jax
import jax.numpy as jnp
from jax import lax
from jax.experimental import pallas as pl
from jax.experimental.pallas import tpu as pltpu
from jax.sharding import PartitionSpec as P

HEAD_DIM = 128
G = 4
BLK = 64
NEG = -1e30
THETA = 500000.0
MESH = pl.DeviceIdType.MESH
F32 = jnp.float32
BF16 = jnp.bfloat16
FAR = 1 << 30
DRAFT_ROWS = 16

PHASES = ((0, 1), (2, 3, 4, 5), (6, 7))
EXTRA = (160, 160)
UNITS_A = {3: (0, 1), 4: (1, 2), 5: (2, 3), 6: (3, 4), 7: (4, 5), 8: (5, 6)}
LATE_A = {1: (6, 7), 2: (7, 8)}
CACHE_AT = 2
UNITS_B = {3: (0, 1), 4: (1, 2), 5: (2, 3), 6: (3, 4), 7: (4, 5), 8: (5, 6)}
LATE_B = {1: (6, 7), 2: (7, 8)}
QUERY_AT = 2
UNITS_C = {3: (0, 2), 4: (2, 4), 5: (4, 5), 6: (5, 6), 7: (6, 7), 8: (7, 8)}


def rope_tables(pos):
    lane = lax.broadcasted_iota(jnp.int32, (pos.shape[0], HEAD_DIM), 1)
    half = HEAD_DIM // 2
    pair = jnp.where(lane < half, lane, lane - half).astype(F32)
    freq = jnp.exp(pair * (-math.log(THETA) / half))
    angle = pos.astype(F32) * freq
    sine = jnp.sin(angle)
    return jnp.cos(angle), jnp.where(lane < half, -sine, sine)


def rope(v, cosine, sine):
    return v * cosine + pltpu.roll(v, HEAD_DIM // 2, 1) * sine


def bounds(table, s):
    if isinstance(s, int):
        return table.get(s, (0, 0))
    low, high = jnp.int32(0), jnp.int32(0)
    for k, (a, b) in table.items():
        low = jnp.where(s == k, a, low)
        high = jnp.where(s == k, b, high)
    return low, high


def over(table, s, f):
    low, high = bounds(table, s)
    if isinstance(s, int) and low == high:
        return

    def one(u, _):
        f(u)
        return 0

    lax.fori_loop(low, high, one, 0)


def kernel(
    groups, shards, heads, pairs,
    x_hbm, d_ref, wq_hbm, wk_hbm, wv_hbm, wo_hbm, map_ref, len_ref, owner_ref,
    out_hbm, dattn_ref, dec_ref,
    buf, xin, xs, dbuf, acc, qbuf, mbuf, lbuf, obuf, limit, ostage, oready, cosb, sinb, dcos, dsin, kpos,
    dkv, aflat, lhs, wo, part, parts,
    load_sem, x_sem, out_sem, send_sem, recv_sem, ysend_sem, yrecv_sem, dsend_sem, drecv_sem, psend_sem, precv_sem,
):
    me = lax.axis_index("shard")
    head = lax.axis_index("head")
    pair = lax.axis_index("pair")
    group = lax.axis_index("groups")
    right = lax.rem(me + 1, shards)
    left = lax.rem(me + shards - 1, shards)
    odd = lax.rem(group, 2)
    twin = group + 1 - 2 * odd
    far = shards // 2
    rows, seqs, width = x_hbm.shape
    depth = wq_hbm.shape[0]
    steps = d_ref.shape[0]
    tall = rows * seqs
    drafts = steps * seqs
    per = rows // BLK
    scale = 1.0 / math.sqrt(HEAD_DIM)
    factor = scale * math.log2(math.e)
    peers = heads * pairs
    place = head * pairs + pair
    high = G * rows + DRAFT_ROWS

    barrier = pltpu.get_barrier_semaphore()
    for z in (left, right):
        pl.semaphore_signal(barrier, inc=1, device_id={"shard": z}, device_id_type=MESH)
    pl.semaphore_signal(barrier, inc=1, device_id={"groups": twin}, device_id_type=MESH)
    for k in range(1, peers):
        other = lax.rem(place + k, peers)
        pl.semaphore_signal(
            barrier, inc=1, device_id={"head": other // pairs, "pair": other % pairs}, device_id_type=MESH
        )

    def owner_of(v):
        half = (v + 1) // 2
        return lax.rem(me + shards + jnp.where(lax.rem(v, 2) == 1, -half, half), shards)

    sources = [wk_hbm, wv_hbm] + [wq_hbm.at[:, g * HEAD_DIM : (g + 1) * HEAD_DIM] for g in range(G)]
    loads = [pltpu.make_async_copy(src, buf.at[s, me], load_sem.at[s]) for s, src in enumerate(sources)]
    wo_load = pltpu.make_async_copy(wo_hbm, wo, load_sem.at[6])

    def x_load(owner):
        return pltpu.make_async_copy(
            x_hbm.at[:, :, pl.ds(pl.multiple_of(owner * depth, depth), depth)], xin.at[owner], x_sem.at[owner]
        )

    for load in loads:
        load.start()

    def start_x(v, _):
        x_load(owner_of(v)).start()
        return 0

    lax.fori_loop(0, shards, start_x, 0)
    wo_load.start()

    d_all = d_ref[...].astype(F32)
    dbuf[me] = jnp.concatenate([d_all[t] for t in range(steps)], 0).astype(BF16)

    pl.semaphore_wait(barrier, 2 + 1 + peers - 1)

    def items(phase):
        if phase == 2:
            return [(0, 0, depth // 2), (1, depth // 2, depth // 2)]
        extra = EXTRA[phase]
        found = [(0, odd * (depth - extra), extra)]
        if 2 * extra < depth:
            found.append((1, extra, depth - 2 * extra))
        return found

    def hop(stream, item, way, s):
        index, first, count = item
        owner = lax.rem(me + shards - (s - 1), shards) if way == 0 else lax.rem(me + (s - 1), shards)
        if isinstance(s, int) and s == far:
            count = count // 2
            first = first + way * count
        if not isinstance(first, int):
            first = pl.multiple_of(first, 16)
        ref = buf.at[stream, owner, pl.ds(first, count)]
        lane = stream * 4 + index * 2 + way
        return pltpu.make_async_remote_copy(
            src_ref=ref, dst_ref=ref, send_sem=send_sem.at[lane], recv_sem=recv_sem.at[lane, s - 1],
            device_id={"shard": right if way == 0 else left}, device_id_type=MESH,
        )

    def hand(stream, v):
        extra = EXTRA[0 if stream in PHASES[0] else 1]
        ref = buf.at[stream, owner_of(v), pl.ds(pl.multiple_of(odd * (depth - extra), 16), extra)]
        return pltpu.make_async_remote_copy(
            src_ref=ref, dst_ref=ref, send_sem=ysend_sem.at[stream, v], recv_sem=yrecv_sem.at[stream, v],
            device_id={"groups": twin}, device_id_type=MESH,
        )

    def draft_hop(way, s):
        owner = lax.rem(me + shards - (s - 1), shards) if way == 0 else lax.rem(me + (s - 1), shards)
        return pltpu.make_async_remote_copy(
            src_ref=dbuf.at[owner], dst_ref=dbuf.at[owner], send_sem=dsend_sem.at[way],
            recv_sem=drecv_sem.at[way, s - 1], device_id={"shard": right if way == 0 else left}, device_id_type=MESH,
        )

    def launch(phase):
        for item in items(phase):
            for stream in PHASES[phase]:
                for way in range(2):
                    hop(stream, item, way, 1).start()
        if phase == 0:
            for way in range(2):
                draft_hop(way, 1).start()

    def pass_on(phase, s):
        for item in items(phase):
            for stream in PHASES[phase]:
                for way in range(2):
                    hop(stream, item, way, s).wait_recv()
                    hop(stream, item, way, s).wait_send()

                    @pl.when(s < far - 1)
                    def _():
                        hop(stream, item, way, s + 1).start()

                    @pl.when(s == far - 1)
                    def _():
                        hop(stream, item, way, far).start()

                    if phase < 2 and item[0] == 0:
                        hand(stream, 2 * s - 1 + way).start()
        if phase == 0:
            for way in range(2):
                draft_hop(way, s).wait_recv()
                draft_hop(way, s).wait_send()

            draft_hop(0, s + 1).start()

            @pl.when(s < far - 1)
            def _():
                draft_hop(1, s + 1).start()

    def finish(phase):
        for item in items(phase):
            for stream in PHASES[phase]:
                for way in range(2):
                    hop(stream, item, way, far).wait_recv()
                    hop(stream, item, way, far).wait_send()
                if phase < 2 and item[0] == 0:
                    hand(stream, 2 * far - 1).start()
        if phase == 0:
            draft_hop(0, far).wait_recv()
            draft_hop(0, far).wait_send()

    def ring(phase, work, ready_next):
        def step(s, _):
            pass_on(phase, s)
            work(s)
            return 0

        lax.fori_loop(1, far, step, 0)
        ready_next()
        finish(phase)
        work(far)

    def multiply(phase, u):
        streams = PHASES[phase]

        def one(v, _):
            owner = owner_of(v)
            if phase == 0:
                x_load(owner).wait()
                xs[owner, 0:tall] = xin[owner].reshape(tall, depth)
                xs[owner, tall : tall + drafts] = dbuf[owner]

            @pl.when(v > 0)
            def _():
                for stream in streams:
                    hand(stream, v).wait_recv()

            w = jnp.concatenate([buf[stream, owner] for stream in streams], 1)
            got = jnp.dot(xs[owner], w, preferred_element_type=F32)
            for k, stream in enumerate(streams):
                acc[stream] += got[:, k * HEAD_DIM : (k + 1) * HEAD_DIM]
            return 0

        lax.fori_loop(2 * u, 2 * u + 2, one, 0)

    def own_rows(count):
        row = lax.rem(lax.broadcasted_iota(jnp.int32, (count, 1), 0), rows)
        pos = row + map_ref[me * per] * BLK
        for j in range(1, per):
            pos = jnp.where(row >= j * BLK, row - j * BLK + map_ref[me * per + j] * BLK, pos)
        return pos

    loads[0].wait()
    loads[1].wait()
    launch(0)

    for stream in range(6):
        acc[stream] = jnp.zeros(acc.shape[1:], F32)
    cosb[...], sinb[...] = rope_tables(own_rows(rows))
    drow = lax.broadcasted_iota(jnp.int32, (drafts, 1), 0)
    dpos = jnp.zeros((drafts, 1), jnp.int32)
    for t in range(steps):
        for b in range(seqs):
            dpos = jnp.where(drow == t * seqs + b, len_ref[b] + t, dpos)
    dcos[...], dsin[...] = rope_tables(dpos)
    seq = lax.broadcasted_iota(jnp.int32, (seqs, rows), 0)
    lengths = jnp.zeros((seqs, rows), jnp.int32)
    for b in range(seqs):
        lengths = jnp.where(seq == b, len_ref[b], lengths)

    def positions(z, _):
        lane = lax.broadcasted_iota(jnp.int32, (seqs, rows), 1)
        where = lane + map_ref[z * per] * BLK
        for j in range(1, per):
            where = jnp.where(lane >= j * BLK, lane - j * BLK + map_ref[z * per + j] * BLK, where)
        kpos[z] = jnp.where(where < lengths, where, FAR)
        return 0

    lax.fori_loop(0, shards, positions, 0)
    limit[0 : G * rows] = jnp.broadcast_to(own_rows(G * rows), (G * rows, HEAD_DIM))
    limit[G * rows : high] = jnp.full((DRAFT_ROWS, HEAD_DIM), FAR - 1, jnp.int32)

    def next0():
        for load in loads[2:]:
            load.wait()
        launch(1)

    ring(0, lambda s: over(UNITS_A, s, functools.partial(multiply, 0)), next0)

    def own_cache():
        def one(b, _):
            k = acc[0, pl.ds(b, rows, stride=seqs), :]
            v = acc[1, pl.ds(b, rows, stride=seqs), :]
            at = pl.ds(pl.multiple_of(b * rows, rows), rows)
            buf[6, me, at] = rope(k, cosb[...], sinb[...]).astype(BF16)
            buf[7, me, at] = v.astype(BF16)
            return 0

        lax.fori_loop(0, seqs, one, 0)
        dkv[0] = rope(acc[0, tall : tall + drafts, :], dcos[...], dsin[...]).astype(BF16)
        dkv[1] = acc[1, tall : tall + drafts, :].astype(BF16)

    def work1(s):
        if not isinstance(s, int):
            over(LATE_A, s, functools.partial(multiply, 0))
            pl.when(s == CACHE_AT)(own_cache)
        over(UNITS_B, s, functools.partial(multiply, 1))

    ring(1, work1, lambda: launch(2))

    def queries():
        dq = [rope(acc[2 + g, tall : tall + drafts, :], dcos[...], dsin[...]) for g in range(G)]
        for b in range(seqs):
            pieces = [dq[g][t * seqs + b : t * seqs + b + 1] for g in range(G) for t in range(steps)]
            pieces.append(jnp.zeros((DRAFT_ROWS - G * steps, HEAD_DIM), F32))
            qbuf[b, G * rows : high] = jnp.concatenate(pieces, 0).astype(BF16)

        def one(b, _):
            for g in range(G):
                q = acc[2 + g, pl.ds(b, rows, stride=seqs), :]
                qbuf[b, g * rows : (g + 1) * rows] = rope(q, cosb[...], sinb[...]).astype(BF16)
            mbuf[b] = jnp.full((high, HEAD_DIM), NEG, F32)
            lbuf[b] = jnp.zeros((high, HEAD_DIM), F32)
            obuf[b] = jnp.zeros((high, HEAD_DIM), F32)
            return 0

        lax.fori_loop(0, seqs, one, 0)

    def attend(u):
        first, second = owner_of(2 * u), owner_of(2 * u + 1)

        def one(b, _):
            at = pl.ds(pl.multiple_of(b * rows, rows), rows)
            k = jnp.concatenate([buf[6, first, at, :], buf[6, second, at, :]], 0)
            v = jnp.concatenate([buf[7, first, at, :], buf[7, second, at, :]], 0)
            kp0 = kpos[first, pl.ds(b, 1), :]
            kp1 = kpos[second, pl.ds(b, 1), :]
            tile = high // 3
            for r in range(0, high, tile):
                at_r = slice(r, r + tile)
                s = lax.dot_general(qbuf[b, at_r], k, (((1,), (1,)), ((), ())), preferred_element_type=F32)
                most = limit[at_r]
                s0 = jnp.where(kp0 <= most, s[:, 0:rows], NEG)
                s1 = jnp.where(kp1 <= most, s[:, rows : 2 * rows], NEG)
                before = mbuf[b, at_r]
                top = jnp.maximum(before, jnp.max(jnp.maximum(s0, s1), 1, keepdims=True))
                shrink = jnp.exp2((before - top) * factor)
                w0 = jnp.exp2((s0 - top) * factor)
                w1 = jnp.exp2((s1 - top) * factor)
                mbuf[b, at_r] = top
                lbuf[b, at_r] = lbuf[b, at_r] * shrink + (w0 + w1)
                w = jnp.concatenate([w0, w1], 1).astype(BF16)
                obuf[b, at_r] = obuf[b, at_r] * shrink + jnp.dot(w, v, preferred_element_type=F32)
            return 0

        lax.fori_loop(0, seqs, one, 0)

    def work2(s):
        if not isinstance(s, int):
            over(LATE_B, s, functools.partial(multiply, 1))
            pl.when(s == QUERY_AT)(queries)
        over(UNITS_C, s, attend)

    ring(2, work2, lambda: None)

    wo_load.wait()
    r = lax.broadcasted_iota(jnp.int32, (DRAFT_ROWS, drafts), 0)
    c = lax.broadcasted_iota(jnp.int32, (DRAFT_ROWS, drafts), 1)
    for b in range(seqs):
        at_r = slice(G * rows, high)
        new = lax.dot_general(qbuf[b, at_r], dkv[0], (((1,), (1,)), ((), ())), preferred_element_type=F32)
        seen = (lax.rem(c, seqs) == b) & (c // seqs <= lax.rem(r, steps))
        new = jnp.where(seen, new, NEG)
        before = mbuf[b, at_r][:, 0:1]
        top = jnp.maximum(before, jnp.max(new, 1, keepdims=True))
        shrink = jnp.exp2((before - top) * factor)
        w = jnp.where(seen, jnp.exp2((new - top) * factor), 0.0)
        total = jnp.sum(lbuf[b, at_r], 1, keepdims=True) * shrink + jnp.sum(w, 1, keepdims=True)
        mixed = obuf[b, at_r] * shrink + jnp.dot(w.astype(BF16), dkv[1], preferred_element_type=F32)
        attn = (mixed / total).astype(BF16).astype(F32)
        aflat[b * G * steps : (b + 1) * G * steps] = attn[0 : G * steps]
    for g in range(G):
        for t in range(steps):
            lhs[t * seqs : (t + 1) * seqs, g * HEAD_DIM : (g + 1) * HEAD_DIM] = aflat[
                pl.ds(g * steps + t, seqs, stride=G * steps), :
            ]
    partial = jnp.dot(lhs[...].astype(BF16), wo[...], preferred_element_type=F32)
    wide = partial.shape[1] // heads
    for h in range(heads):
        part[h] = partial[:, h * wide : (h + 1) * wide]
    parts[place] = part[head]

    def give(k):
        other = lax.rem(place + k, peers)
        return pltpu.make_async_remote_copy(
            src_ref=part.at[other // pairs], dst_ref=parts.at[place], send_sem=psend_sem.at[k], recv_sem=precv_sem.at[k],
            device_id={"head": other // pairs, "pair": other % pairs}, device_id_type=MESH,
        )

    r1 = lax.broadcasted_iota(jnp.int32, (seqs * G * steps, 1), 0)
    mine = jnp.zeros((seqs * G * steps, 1), jnp.int32)
    for p in range(seqs * G):
        mine = jnp.where(r1 // steps == p, owner_ref[0, p], mine)
    picked = jnp.where(mine == me, aflat[...], 0.0)
    for t in range(steps):
        dattn_ref[t, 0] = jnp.sum(
            jnp.where(lax.rem(r1, steps) == t, picked, 0.0), 0, keepdims=True
        ).astype(BF16)

    for k in range(1, peers):
        give(k).start()

    def put(b, _):
        for g in range(G):
            at_g = slice(g * rows, (g + 1) * rows)
            total = jnp.sum(lbuf[b, at_g], 1, keepdims=True)
            ostage[g, pl.ds(b, rows, stride=seqs), :] = obuf[b, at_g] / total
        return 0

    lax.fori_loop(0, seqs, put, 0)
    for g in range(G):
        oready[:, :, g * HEAD_DIM : (g + 1) * HEAD_DIM] = ostage[g].astype(BF16).reshape(rows, seqs, HEAD_DIM)
    store = pltpu.make_async_copy(oready, out_hbm, out_sem.at[0])
    store.start()

    for k in range(1, peers):
        give(k).wait_recv()
    summed = jnp.sum(parts[...], 0)
    narrow = wide // pairs
    got = summed[:, 0:narrow]
    for j in range(1, pairs):
        got = jnp.where(pair == j, summed[:, j * narrow : (j + 1) * narrow], got)
    for t in range(steps):
        dec_ref[t] = got[t * seqs : (t + 1) * seqs].astype(BF16)

    for k in range(1, peers):
        give(k).wait_send()

    def drain(v, _):
        for stream in range(6):
            hand(stream, v).wait_send()
        return 0

    lax.fori_loop(1, shards, drain, 0)
    store.wait()


def body(groups, shards, heads, pairs, x, d, wq, wk, wv, wo, block_map, prompt_len, owner):
    rows, seqs, width = x.shape
    depth = wq.shape[0]
    steps = d.shape[0]
    drafts = steps * seqs
    tall = rows * seqs
    peers = heads * pairs
    high = G * rows + DRAFT_ROWS
    any_ = pl.BlockSpec(memory_space=pl.ANY)
    vmem = pl.BlockSpec(memory_space=pltpu.VMEM)
    smem = pl.BlockSpec(memory_space=pltpu.SMEM)
    dma = pltpu.SemaphoreType.DMA
    return pl.pallas_call(
        functools.partial(kernel, groups, shards, heads, pairs),
        out_shape=(
            jax.ShapeDtypeStruct((rows, seqs, wq.shape[1]), BF16),
            jax.ShapeDtypeStruct((steps, 1, 1, HEAD_DIM), BF16),
            jax.ShapeDtypeStruct((steps, seqs, wo.shape[1] // peers), BF16),
        ),
        in_specs=[any_, vmem, any_, any_, any_, any_, smem, smem, smem],
        out_specs=(any_, vmem, vmem),
        scratch_shapes=[
            pltpu.VMEM((8, shards, depth, HEAD_DIM), BF16),
            pltpu.VMEM((shards, rows, seqs, depth), BF16),
            pltpu.VMEM((shards, tall + drafts, depth), BF16),
            pltpu.VMEM((shards, drafts, depth), BF16),
            pltpu.VMEM((6, tall + drafts, HEAD_DIM), F32),
            pltpu.VMEM((seqs, high, HEAD_DIM), BF16),
            pltpu.VMEM((seqs, high, HEAD_DIM), F32),
            pltpu.VMEM((seqs, high, HEAD_DIM), F32),
            pltpu.VMEM((seqs, high, HEAD_DIM), F32),
            pltpu.VMEM((high, HEAD_DIM), jnp.int32),
            pltpu.VMEM((G, tall, HEAD_DIM), F32),
            pltpu.VMEM((rows, seqs, wq.shape[1]), BF16),
            pltpu.VMEM((rows, HEAD_DIM), F32),
            pltpu.VMEM((rows, HEAD_DIM), F32),
            pltpu.VMEM((drafts, HEAD_DIM), F32),
            pltpu.VMEM((drafts, HEAD_DIM), F32),
            pltpu.VMEM((shards, seqs, rows), jnp.int32),
            pltpu.VMEM((2, drafts, HEAD_DIM), BF16),
            pltpu.VMEM((seqs * G * steps, HEAD_DIM), F32),
            pltpu.VMEM((drafts, wq.shape[1]), F32),
            pltpu.VMEM(wo.shape, BF16),
            pltpu.VMEM((heads, drafts, wo.shape[1] // heads), F32),
            pltpu.VMEM((peers, drafts, wo.shape[1] // heads), F32),
            dma((7,)),
            dma((shards,)),
            dma((1,)),
            dma((32,)),
            dma((32, shards // 2)),
            dma((6, shards)),
            dma((6, shards)),
            dma((2,)),
            dma((2, shards // 2)),
            dma((peers,)),
            dma((peers,)),
        ],
        compiler_params=pltpu.CompilerParams(
            collective_id=0, has_side_effects=True, vmem_limit_bytes=60 * 1024 * 1024
        ),
    )(x, d, wq, wk, wv, wo, block_map, prompt_len, owner)


def solution(mesh):
    placed = (
        P("shard", "groups", None),
        P(None, "groups", "shard"),
        P("shard", ("head", "pair")),
        P("shard", ("head", "pair")),
        P("shard", ("head", "pair")),
        P(("head", "pair"), "shard"),
        P("groups"),
        P("groups"),
        P(("head", "pair"), "groups"),
    )
    sizes = [mesh.shape[name] for name in ("groups", "shard", "head", "pair")]
    return jax.shard_map(
        functools.partial(body, *sizes),
        mesh=mesh,
        in_specs=placed,
        out_specs=(
            P("shard", "groups", ("head", "pair")),
            P(None, ("groups", "shard"), ("head", "pair"), None),
            P(None, "groups", ("shard", "head", "pair")),
        ),
        check_vma=False,
    )
```

```python
import functools
import math

import jax
import jax.numpy as jnp
from jax import lax
from jax.experimental import pallas as pl
from jax.experimental.pallas import tpu as pltpu
from jax.sharding import PartitionSpec as P

HEAD_DIM = 128
G = 4
BLK = 64
NEG = -1e30
THETA = 500000.0
MESH = pl.DeviceIdType.MESH
F32 = jnp.float32
BF16 = jnp.bfloat16
FAR = 1 << 30
DRAFT_ROWS = 16

PHASES = ((0, 1), (2, 3, 4, 5), (6, 7))
EXTRA = (176, 208)
PARTS = (((0, 1, True), (1, 1, True), (0, 1, False), (1, 1, False)), ((2, 2, True), (4, 2, True), (2, 4, False)))
LANES = (0, 8, 0)
TURNS = 4
UNITS_A = {3: (0, 1), 4: (1, 2), 5: (2, 3), 6: (3, 4), 7: (4, 5), 8: (5, 6)}
LATE_A = {1: (6, 7), 2: (7, 8)}
CACHE_AT = 2
UNITS_B = {3: (0, 1), 4: (1, 2), 5: (2, 3), 6: (3, 4), 8: (4, 5)}
LATE_B = {1: (5, 6), 3: (6, 7), 4: (7, 8)}
QUERY_AT = 4
UNITS_C = {4: (0, 1), 5: (1, 3), 6: (3, 5), 7: (5, 7)}


def rope_tables(pos):
    lane = lax.broadcasted_iota(jnp.int32, (pos.shape[0], HEAD_DIM), 1)
    half = HEAD_DIM // 2
    pair = jnp.where(lane < half, lane, lane - half).astype(F32)
    freq = jnp.exp(pair * (-math.log(THETA) / half))
    angle = pos.astype(F32) * freq
    sine = jnp.sin(angle)
    return jnp.cos(angle), jnp.where(lane < half, -sine, sine)


def rope(v, cosine, sine):
    return v * cosine + pltpu.roll(v, HEAD_DIM // 2, 1) * sine


def bounds(table, s):
    if isinstance(s, int):
        return table.get(s, (0, 0))
    low, high = jnp.int32(0), jnp.int32(0)
    for k, (a, b) in table.items():
        low = jnp.where(s == k, a, low)
        high = jnp.where(s == k, b, high)
    return low, high


def over(table, s, f):
    low, high = bounds(table, s)
    if isinstance(s, int) and low == high:
        return

    def one(u, _):
        f(u)
        return 0

    lax.fori_loop(low, high, one, 0)


def kernel(
    groups, shards, heads, pairs,
    x_hbm, d_ref, wq_hbm, wk_hbm, wv_hbm, wo_hbm, map_ref, len_ref, owner_ref,
    out_hbm, dattn_ref, dec_ref,
    buf, xin, xs, dbuf, acc, qbuf, mbuf, lbuf, obuf, limit, ostage, oready, cosb, sinb, dcos, dsin, kpos,
    dkv, aflat, lhs, wo, part, parts,
    load_sem, x_sem, out_sem, send_sem, recv_sem, ysend_sem, yrecv_sem, dsend_sem, drecv_sem, psend_sem, precv_sem,
):
    me = lax.axis_index("shard")
    head = lax.axis_index("head")
    pair = lax.axis_index("pair")
    group = lax.axis_index("groups")
    right = lax.rem(me + 1, shards)
    left = lax.rem(me + shards - 1, shards)
    odd = lax.rem(group, 2)
    twin = group + 1 - 2 * odd
    far = shards // 2
    rows, seqs, width = x_hbm.shape
    depth = wq_hbm.shape[0]
    steps = d_ref.shape[0]
    tall = rows * seqs
    drafts = steps * seqs
    per = rows // BLK
    scale = 1.0 / math.sqrt(HEAD_DIM)
    factor = scale * math.log2(math.e)
    peers = heads * pairs
    place = head * pairs + pair
    high = G * rows + DRAFT_ROWS

    barrier = pltpu.get_barrier_semaphore()
    for z in (left, right):
        pl.semaphore_signal(barrier, inc=1, device_id={"shard": z}, device_id_type=MESH)
    pl.semaphore_signal(barrier, inc=1, device_id={"groups": twin}, device_id_type=MESH)
    for k in range(1, peers):
        other = lax.rem(place + k, peers)
        pl.semaphore_signal(
            barrier, inc=1, device_id={"head": other // pairs, "pair": other % pairs}, device_id_type=MESH
        )

    def owner_of(v):
        half = (v + 1) // 2
        return lax.rem(me + shards + jnp.where(lax.rem(v, 2) == 1, -half, half), shards)

    sources = [wk_hbm, wv_hbm] + [wq_hbm.at[:, g * HEAD_DIM : (g + 1) * HEAD_DIM] for g in range(G)]
    loads = [pltpu.make_async_copy(src, buf.at[s, me], load_sem.at[s]) for s, src in enumerate(sources)]
    wo_load = pltpu.make_async_copy(wo_hbm, wo, load_sem.at[6])

    def x_load(owner):
        return pltpu.make_async_copy(
            x_hbm.at[:, :, pl.ds(pl.multiple_of(owner * depth, depth), depth)], xin.at[owner], x_sem.at[owner]
        )

    for load in loads:
        load.start()

    def start_x(v, _):
        x_load(owner_of(v)).start()
        return 0

    lax.fori_loop(0, shards, start_x, 0)
    wo_load.start()

    d_all = d_ref[...].astype(F32)
    dbuf[me] = jnp.concatenate([d_all[t] for t in range(steps)], 0).astype(BF16)

    pl.semaphore_wait(barrier, 2 + 1 + peers - 1)

    def pieces(phase):
        if phase == 2:
            found = [(6 + k % 2, 1, k // 2 * (depth // 2), depth // 2, False) for k in range(4)]
        else:
            extra = EXTRA[phase]
            found = [
                (stream, count, odd * (depth - extra), extra, True) if own else (stream, count, extra, depth - 2 * extra, False)
                for stream, count, own in PARTS[phase]
            ]
        return [(LANES[phase] + 2 * k, *piece) for k, piece in enumerate(found)]

    def hop(piece, way, s):
        lane, stream, streams, first, count, _ = piece
        owner = lax.rem(me + shards - (s - 1), shards) if way == 0 else lax.rem(me + (s - 1), shards)
        if isinstance(s, int) and s == far:
            upper = (count // 2 + 15) // 16 * 16
            first = first + way * upper
            count = count - upper if way else upper
        if not isinstance(first, int):
            first = pl.multiple_of(first, 16)
        ref = buf.at[pl.ds(stream, streams), owner, pl.ds(first, count)]
        turn = (s - 1) % TURNS if isinstance(s, int) else lax.rem(s - 1, TURNS)
        return pltpu.make_async_remote_copy(
            src_ref=ref, dst_ref=ref, send_sem=send_sem.at[lane + way], recv_sem=recv_sem.at[lane + way, turn],
            device_id={"shard": right if way == 0 else left}, device_id_type=MESH,
        )

    def hand(phase, v):
        extra = EXTRA[phase]
        streams = PHASES[phase]
        ref = buf.at[
            pl.ds(streams[0], len(streams)), owner_of(v), pl.ds(pl.multiple_of(odd * (depth - extra), 16), extra)
        ]
        return pltpu.make_async_remote_copy(
            src_ref=ref, dst_ref=ref, send_sem=ysend_sem.at[phase, v], recv_sem=yrecv_sem.at[phase, v],
            device_id={"groups": twin}, device_id_type=MESH,
        )

    def draft_hop(way, s):
        owner = lax.rem(me + shards - (s - 1), shards) if way == 0 else lax.rem(me + (s - 1), shards)
        return pltpu.make_async_remote_copy(
            src_ref=dbuf.at[owner], dst_ref=dbuf.at[owner], send_sem=dsend_sem.at[way],
            recv_sem=drecv_sem.at[way, s - 1], device_id={"shard": right if way == 0 else left}, device_id_type=MESH,
        )

    def launch(phase):
        for piece in pieces(phase):
            for way in range(2):
                hop(piece, way, 1).start()
        if phase == 0:
            for way in range(2):
                draft_hop(way, 1).start()

    def pass_on(phase, s):
        found = pieces(phase)
        owns = sum(piece[-1] for piece in found)
        for k, piece in enumerate(found):
            for way in range(2):
                hop(piece, way, s).wait_recv()
                hop(piece, way, s).wait_send()

                @pl.when(s < far - 1)
                def _():
                    hop(piece, way, s + 1).start()

                @pl.when(s == far - 1)
                def _():
                    hop(piece, way, far).start()

                if k == owns - 1:
                    hand(phase, 2 * s - 1 + way).start()
        if phase == 0:
            for way in range(2):
                draft_hop(way, s).wait_recv()
                draft_hop(way, s).wait_send()

            draft_hop(0, s + 1).start()

            @pl.when(s < far - 1)
            def _():
                draft_hop(1, s + 1).start()

    def finish(phase):
        found = pieces(phase)
        owns = sum(piece[-1] for piece in found)
        for k, piece in enumerate(found):
            for way in range(2):
                hop(piece, way, far).wait_recv()
                hop(piece, way, far).wait_send()
            if k == owns - 1:
                hand(phase, 2 * far - 1).start()
        if phase == 0:
            draft_hop(0, far).wait_recv()
            draft_hop(0, far).wait_send()

    def ring(phase, work, ready_next):
        def step(s, _):
            pass_on(phase, s)
            work(s)
            return 0

        lax.fori_loop(1, far, step, 0)
        ready_next()
        finish(phase)
        work(far)

    def multiply(phase, u):
        streams = PHASES[phase]

        def one(v, _):
            owner = owner_of(v)
            if phase == 0:
                x_load(owner).wait()
                xs[owner, 0:tall] = xin[owner].reshape(tall, depth)
                xs[owner, tall : tall + drafts] = dbuf[owner]

            @pl.when(v > 0)
            def _():
                hand(phase, v).wait_recv()

            w = jnp.concatenate([buf[stream, owner] for stream in streams], 1)
            got = jnp.dot(xs[owner], w, preferred_element_type=F32)
            for k, stream in enumerate(streams):
                acc[stream] += got[:, k * HEAD_DIM : (k + 1) * HEAD_DIM]
            return 0

        lax.fori_loop(2 * u, 2 * u + 2, one, 0)

    def own_rows(count):
        row = lax.rem(lax.broadcasted_iota(jnp.int32, (count, 1), 0), rows)
        pos = row + map_ref[me * per] * BLK
        for j in range(1, per):
            pos = jnp.where(row >= j * BLK, row - j * BLK + map_ref[me * per + j] * BLK, pos)
        return pos

    loads[0].wait()
    loads[1].wait()
    launch(0)

    for stream in range(6):
        acc[stream] = jnp.zeros(acc.shape[1:], F32)
    cosb[...], sinb[...] = rope_tables(own_rows(rows))
    drow = lax.broadcasted_iota(jnp.int32, (drafts, 1), 0)
    dpos = jnp.zeros((drafts, 1), jnp.int32)
    for t in range(steps):
        for b in range(seqs):
            dpos = jnp.where(drow == t * seqs + b, len_ref[b] + t, dpos)
    dcos[...], dsin[...] = rope_tables(dpos)
    seq = lax.broadcasted_iota(jnp.int32, (seqs, rows), 0)
    lengths = jnp.zeros((seqs, rows), jnp.int32)
    for b in range(seqs):
        lengths = jnp.where(seq == b, len_ref[b], lengths)

    def positions(z, _):
        lane = lax.broadcasted_iota(jnp.int32, (seqs, rows), 1)
        where = lane + map_ref[z * per] * BLK
        for j in range(1, per):
            where = jnp.where(lane >= j * BLK, lane - j * BLK + map_ref[z * per + j] * BLK, where)
        kpos[z] = jnp.where(where < lengths, where, FAR)
        return 0

    lax.fori_loop(0, shards, positions, 0)
    limit[0 : G * rows] = jnp.broadcast_to(own_rows(G * rows), (G * rows, HEAD_DIM))
    limit[G * rows : high] = jnp.full((DRAFT_ROWS, HEAD_DIM), FAR - 1, jnp.int32)

    def next0():
        for load in loads[2:]:
            load.wait()
        launch(1)

    ring(0, lambda s: over(UNITS_A, s, functools.partial(multiply, 0)), next0)

    def own_cache():
        def one(b, _):
            k = acc[0, pl.ds(b, rows, stride=seqs), :]
            v = acc[1, pl.ds(b, rows, stride=seqs), :]
            at = pl.ds(pl.multiple_of(b * rows, rows), rows)
            buf[6, me, at] = rope(k, cosb[...], sinb[...]).astype(BF16)
            buf[7, me, at] = v.astype(BF16)
            return 0

        lax.fori_loop(0, seqs, one, 0)
        dkv[0] = rope(acc[0, tall : tall + drafts, :], dcos[...], dsin[...]).astype(BF16)
        dkv[1] = acc[1, tall : tall + drafts, :].astype(BF16)

    def work1(s):
        if not isinstance(s, int):
            over(LATE_A, s, functools.partial(multiply, 0))
            pl.when(s == CACHE_AT)(own_cache)
        over(UNITS_B, s, functools.partial(multiply, 1))

    ring(1, work1, lambda: launch(2))

    def queries():
        dq = [rope(acc[2 + g, tall : tall + drafts, :], dcos[...], dsin[...]) for g in range(G)]
        for b in range(seqs):
            pieces = [dq[g][t * seqs + b : t * seqs + b + 1] for g in range(G) for t in range(steps)]
            pieces.append(jnp.zeros((DRAFT_ROWS - G * steps, HEAD_DIM), F32))
            qbuf[b, G * rows : high] = jnp.concatenate(pieces, 0).astype(BF16)

        def one(b, _):
            for g in range(G):
                q = acc[2 + g, pl.ds(b, rows, stride=seqs), :]
                qbuf[b, g * rows : (g + 1) * rows] = rope(q, cosb[...], sinb[...]).astype(BF16)
            mbuf[b] = jnp.full((high, HEAD_DIM), NEG, F32)
            lbuf[b] = jnp.zeros((high, HEAD_DIM), F32)
            obuf[b] = jnp.zeros((high, HEAD_DIM), F32)
            return 0

        lax.fori_loop(0, seqs, one, 0)

    def attend(u, tiles=((0, high // 3), (high // 3, high // 3 * 2), (high // 3 * 2, high))):
        first, second = owner_of(2 * u), owner_of(2 * u + 1)

        def one(b, _):
            at = pl.ds(pl.multiple_of(b * rows, rows), rows)
            k = jnp.concatenate([buf[6, first, at, :], buf[6, second, at, :]], 0)
            v = jnp.concatenate([buf[7, first, at, :], buf[7, second, at, :]], 0)
            kp0 = kpos[first, pl.ds(b, 1), :]
            kp1 = kpos[second, pl.ds(b, 1), :]
            for low, end in tiles:
                at_r = slice(low, end)
                s = lax.dot_general(qbuf[b, at_r], k, (((1,), (1,)), ((), ())), preferred_element_type=F32)
                most = limit[at_r]
                s0 = jnp.where(kp0 <= most, s[:, 0:rows], NEG)
                s1 = jnp.where(kp1 <= most, s[:, rows : 2 * rows], NEG)
                before = mbuf[b, at_r]
                top = jnp.maximum(before, jnp.max(jnp.maximum(s0, s1), 1, keepdims=True))
                shrink = jnp.exp2((before - top) * factor)
                w0 = jnp.exp2((s0 - top) * factor)
                w1 = jnp.exp2((s1 - top) * factor)
                mbuf[b, at_r] = top
                lbuf[b, at_r] = lbuf[b, at_r] * shrink + (w0 + w1)
                w = jnp.concatenate([w0, w1], 1).astype(BF16)
                obuf[b, at_r] = obuf[b, at_r] * shrink + jnp.dot(w, v, preferred_element_type=F32)
            return 0

        lax.fori_loop(0, seqs, one, 0)

    def work2(s):
        if not isinstance(s, int):
            over(LATE_B, s, functools.partial(multiply, 1))
            pl.when(s == QUERY_AT)(queries)
        over(UNITS_C, s, attend)

    ring(2, work2, lambda: None)

    attend(far - 1, ((G * rows, high),))
    wo_load.wait()
    r = lax.broadcasted_iota(jnp.int32, (DRAFT_ROWS, drafts), 0)
    c = lax.broadcasted_iota(jnp.int32, (DRAFT_ROWS, drafts), 1)
    for b in range(seqs):
        at_r = slice(G * rows, high)
        new = lax.dot_general(qbuf[b, at_r], dkv[0], (((1,), (1,)), ((), ())), preferred_element_type=F32)
        seen = (lax.rem(c, seqs) == b) & (c // seqs <= lax.rem(r, steps))
        new = jnp.where(seen, new, NEG)
        before = mbuf[b, at_r][:, 0:1]
        top = jnp.maximum(before, jnp.max(new, 1, keepdims=True))
        shrink = jnp.exp2((before - top) * factor)
        w = jnp.where(seen, jnp.exp2((new - top) * factor), 0.0)
        total = jnp.sum(lbuf[b, at_r], 1, keepdims=True) * shrink + jnp.sum(w, 1, keepdims=True)
        mixed = obuf[b, at_r] * shrink + jnp.dot(w.astype(BF16), dkv[1], preferred_element_type=F32)
        attn = (mixed / total).astype(BF16).astype(F32)
        aflat[b * G * steps : (b + 1) * G * steps] = attn[0 : G * steps]
    for g in range(G):
        for t in range(steps):
            lhs[t * seqs : (t + 1) * seqs, g * HEAD_DIM : (g + 1) * HEAD_DIM] = aflat[
                pl.ds(g * steps + t, seqs, stride=G * steps), :
            ]
    partial = jnp.dot(lhs[...].astype(BF16), wo[...], preferred_element_type=F32)
    wide = partial.shape[1] // heads
    for h in range(heads):
        part[h] = partial[:, h * wide : (h + 1) * wide]
    parts[place] = part[head]

    def give(k):
        other = lax.rem(place + k, peers)
        return pltpu.make_async_remote_copy(
            src_ref=part.at[other // pairs], dst_ref=parts.at[place], send_sem=psend_sem.at[k], recv_sem=precv_sem.at[k],
            device_id={"head": other // pairs, "pair": other % pairs}, device_id_type=MESH,
        )

    r1 = lax.broadcasted_iota(jnp.int32, (seqs * G * steps, 1), 0)
    mine = jnp.zeros((seqs * G * steps, 1), jnp.int32)
    for p in range(seqs * G):
        mine = jnp.where(r1 // steps == p, owner_ref[0, p], mine)
    picked = jnp.where(mine == me, aflat[...], 0.0)
    found = [jnp.sum(jnp.where(lax.rem(r1, steps) == t, picked, 0.0), 0, keepdims=True) for t in range(steps)]
    dattn_ref[0, 0] = jnp.concatenate(found, 0).astype(BF16)

    for k in range(1, peers):
        give(k).start()

    attend(far - 1, ((0, 2 * rows), (2 * rows, 4 * rows)))

    def put(b, _):
        for g in range(G):
            at_g = slice(g * rows, (g + 1) * rows)
            total = jnp.sum(lbuf[b, at_g], 1, keepdims=True)
            ostage[g, pl.ds(b, rows, stride=seqs), :] = obuf[b, at_g] / total
        return 0

    lax.fori_loop(0, seqs, put, 0)
    for g in range(G):
        oready[:, :, g * HEAD_DIM : (g + 1) * HEAD_DIM] = ostage[g].astype(BF16).reshape(rows, seqs, HEAD_DIM)
    store = pltpu.make_async_copy(oready, out_hbm, out_sem.at[0])
    store.start()

    for k in range(1, peers):
        give(k).wait_recv()
    summed = jnp.sum(parts[...], 0)
    narrow = wide // pairs
    got = summed[:, 0:narrow]
    for j in range(1, pairs):
        got = jnp.where(pair == j, summed[:, j * narrow : (j + 1) * narrow], got)
    for t in range(steps):
        dec_ref[t] = got[t * seqs : (t + 1) * seqs].astype(BF16)

    for k in range(1, peers):
        give(k).wait_send()

    def drain(v, _):
        for phase in range(2):
            hand(phase, v).wait_send()
        return 0

    lax.fori_loop(1, shards, drain, 0)
    store.wait()


def settle(*refs):
    for k in range(3):
        refs[3 + k][...] = refs[k][...]


def body(groups, shards, heads, pairs, x, d, wq, wk, wv, wo, block_map, prompt_len, owner):
    rows, seqs, width = x.shape
    depth = wq.shape[0]
    steps = d.shape[0]
    drafts = steps * seqs
    tall = rows * seqs
    peers = heads * pairs
    high = G * rows + DRAFT_ROWS
    any_ = pl.BlockSpec(memory_space=pl.ANY)
    vmem = pl.BlockSpec(memory_space=pltpu.VMEM)
    smem = pl.BlockSpec(memory_space=pltpu.SMEM)
    dma = pltpu.SemaphoreType.DMA
    made = pl.pallas_call(
        functools.partial(kernel, groups, shards, heads, pairs),
        out_shape=(
            jax.ShapeDtypeStruct((rows, seqs, wq.shape[1]), BF16),
            jax.ShapeDtypeStruct((1, 1, steps, HEAD_DIM), BF16),
            jax.ShapeDtypeStruct((steps, seqs, wo.shape[1] // peers), BF16),
        ),
        in_specs=[any_, vmem, any_, any_, any_, any_, smem, smem, smem],
        out_specs=(any_, vmem, vmem),
        scratch_shapes=[
            pltpu.VMEM((8, shards, depth, HEAD_DIM), BF16),
            pltpu.VMEM((shards, rows, seqs, depth), BF16),
            pltpu.VMEM((shards, tall + drafts, depth), BF16),
            pltpu.VMEM((shards, drafts, depth), BF16),
            pltpu.VMEM((6, tall + drafts, HEAD_DIM), F32),
            pltpu.VMEM((seqs, high, HEAD_DIM), BF16),
            pltpu.VMEM((seqs, high, HEAD_DIM), F32),
            pltpu.VMEM((seqs, high, HEAD_DIM), F32),
            pltpu.VMEM((seqs, high, HEAD_DIM), F32),
            pltpu.VMEM((high, HEAD_DIM), jnp.int32),
            pltpu.VMEM((G, tall, HEAD_DIM), F32),
            pltpu.VMEM((rows, seqs, wq.shape[1]), BF16),
            pltpu.VMEM((rows, HEAD_DIM), F32),
            pltpu.VMEM((rows, HEAD_DIM), F32),
            pltpu.VMEM((drafts, HEAD_DIM), F32),
            pltpu.VMEM((drafts, HEAD_DIM), F32),
            pltpu.VMEM((shards, seqs, rows), jnp.int32),
            pltpu.VMEM((2, drafts, HEAD_DIM), BF16),
            pltpu.VMEM((seqs * G * steps, HEAD_DIM), F32),
            pltpu.VMEM((drafts, wq.shape[1]), F32),
            pltpu.VMEM(wo.shape, BF16),
            pltpu.VMEM((heads, drafts, wo.shape[1] // heads), F32),
            pltpu.VMEM((peers, drafts, wo.shape[1] // heads), F32),
            dma((7,)),
            dma((shards,)),
            dma((1,)),
            dma((14,)),
            dma((14, TURNS)),
            dma((2, shards)),
            dma((2, shards)),
            dma((2,)),
            dma((2, shards // 2)),
            dma((peers,)),
            dma((peers,)),
        ],
        compiler_params=pltpu.CompilerParams(
            collective_id=0, has_side_effects=True, vmem_limit_bytes=60 * 1024 * 1024
        ),
    )(x, d, wq, wk, wv, wo, block_map, prompt_len, owner)
    prefill, draft, decode = pl.pallas_call(
        settle,
        out_shape=tuple(jax.ShapeDtypeStruct(a.shape, a.dtype) for a in made),
        in_specs=[vmem] * 3,
        out_specs=(vmem,) * 3,
    )(*made)
    return prefill, draft.transpose(2, 0, 1, 3), decode


def solution(mesh):
    placed = (
        P("shard", "groups", None),
        P(None, "groups", "shard"),
        P("shard", ("head", "pair")),
        P("shard", ("head", "pair")),
        P("shard", ("head", "pair")),
        P(("head", "pair"), "shard"),
        P("groups"),
        P("groups"),
        P(("head", "pair"), "groups"),
    )
    sizes = [mesh.shape[name] for name in ("groups", "shard", "head", "pair")]
    return jax.shard_map(
        functools.partial(body, *sizes),
        mesh=mesh,
        in_specs=placed,
        out_specs=(
            P("shard", "groups", ("head", "pair")),
            P(None, ("groups", "shard"), ("head", "pair"), None),
            P(None, "groups", ("shard", "head", "pair")),
        ),
        check_vma=False,
    )
```

```python
import functools
import math

import jax
import jax.numpy as jnp
from jax import lax
from jax.experimental import pallas as pl
from jax.experimental.pallas import tpu as pltpu
from jax.sharding import PartitionSpec as P

HEAD_DIM = 128
G = 4
BLK = 64
NEG = -1e30
THETA = 500000.0
MESH = pl.DeviceIdType.MESH
F32 = jnp.float32
BF16 = jnp.bfloat16
FAR = 1 << 30
DRAFT_ROWS = 16

PHASES = ((0, 1), (2, 3, 4, 5), (6, 7))
EXTRA = (176, 208)
PARTS = (((0, 1, True), (1, 1, True), (0, 1, False), (1, 1, False)), ((2, 2, True), (4, 2, True), (2, 4, False)))
LANES = (0, 8, 0)
TURNS = 4
ORDER = (
    "A1", "launchB", "A2", "B1", "a0", "A3", "a1", "A4", "B2", "a2", "b0", "A5", "a3", "A6", "B3", "a4", "b1",
    "A7", "A8", "a5", "B4", "B5", "a6", "a7", "cache", "launchC", "b2", "B6", "C1", "b3", "B7", "C2", "b4",
    "B8", "C3", "b5", "C4", "b6", "C5", "b7", "queries", "c0", "C6", "c1", "c2", "c3", "C7", "c4", "c5", "C8",
    "c6",
)


def rope_tables(pos):
    lane = lax.broadcasted_iota(jnp.int32, (pos.shape[0], HEAD_DIM), 1)
    half = HEAD_DIM // 2
    pair = jnp.where(lane < half, lane, lane - half).astype(F32)
    freq = jnp.exp(pair * (-math.log(THETA) / half))
    angle = pos.astype(F32) * freq
    sine = jnp.sin(angle)
    return jnp.cos(angle), jnp.where(lane < half, -sine, sine)


def rope(v, cosine, sine):
    return v * cosine + pltpu.roll(v, HEAD_DIM // 2, 1) * sine


def kernel(
    groups, shards, heads, pairs,
    x_hbm, d_ref, wq_hbm, wk_hbm, wv_hbm, wo_hbm, map_ref, len_ref, owner_ref,
    out_hbm, dattn_ref, dec_ref,
    buf, xin, xs, dbuf, acc, qbuf, mbuf, lbuf, obuf, limit, ostage, oready, cosb, sinb, dcos, dsin, kpos,
    dkv, aflat, lhs, wo, part, parts,
    load_sem, x_sem, out_sem, send_sem, recv_sem, ysend_sem, yrecv_sem, dsend_sem, drecv_sem, psend_sem, precv_sem,
):
    me = lax.axis_index("shard")
    head = lax.axis_index("head")
    pair = lax.axis_index("pair")
    group = lax.axis_index("groups")
    right = lax.rem(me + 1, shards)
    left = lax.rem(me + shards - 1, shards)
    odd = lax.rem(group, 2)
    twin = group + 1 - 2 * odd
    far = shards // 2
    rows, seqs, width = x_hbm.shape
    depth = wq_hbm.shape[0]
    steps = d_ref.shape[0]
    tall = rows * seqs
    drafts = steps * seqs
    per = rows // BLK
    scale = 1.0 / math.sqrt(HEAD_DIM)
    factor = scale * math.log2(math.e)
    peers = heads * pairs
    place = head * pairs + pair
    high = G * rows + DRAFT_ROWS

    barrier = pltpu.get_barrier_semaphore()
    for z in (left, right):
        pl.semaphore_signal(barrier, inc=1, device_id={"shard": z}, device_id_type=MESH)
    pl.semaphore_signal(barrier, inc=1, device_id={"groups": twin}, device_id_type=MESH)
    for k in range(1, peers):
        other = lax.rem(place + k, peers)
        pl.semaphore_signal(
            barrier, inc=1, device_id={"head": other // pairs, "pair": other % pairs}, device_id_type=MESH
        )

    def owner_of(v):
        half = (v + 1) // 2
        return lax.rem(me + shards + jnp.where(lax.rem(v, 2) == 1, -half, half), shards)

    sources = [wk_hbm, wv_hbm] + [wq_hbm.at[:, g * HEAD_DIM : (g + 1) * HEAD_DIM] for g in range(G)]
    loads = [pltpu.make_async_copy(src, buf.at[s, me], load_sem.at[s]) for s, src in enumerate(sources)]
    wo_load = pltpu.make_async_copy(wo_hbm, wo, load_sem.at[6])

    def x_load(owner):
        return pltpu.make_async_copy(
            x_hbm.at[:, :, pl.ds(pl.multiple_of(owner * depth, depth), depth)], xin.at[owner], x_sem.at[owner]
        )

    for load in loads:
        load.start()

    def start_x(v, _):
        x_load(owner_of(v)).start()
        return 0

    lax.fori_loop(0, shards, start_x, 0)
    wo_load.start()

    d_all = d_ref[...].astype(F32)
    dbuf[me] = jnp.concatenate([d_all[t] for t in range(steps)], 0).astype(BF16)

    pl.semaphore_wait(barrier, 2 + 1 + peers - 1)

    def pieces(phase):
        if phase == 2:
            found = [(6 + k % 2, 1, k // 2 * (depth // 2), depth // 2, False) for k in range(4)]
        else:
            extra = EXTRA[phase]
            found = [
                (stream, count, odd * (depth - extra), extra, True) if own else (stream, count, extra, depth - 2 * extra, False)
                for stream, count, own in PARTS[phase]
            ]
        return [(LANES[phase] + 2 * k, *piece) for k, piece in enumerate(found)]

    def hop(piece, way, s):
        lane, stream, streams, first, count, _ = piece
        owner = lax.rem(me + shards - (s - 1), shards) if way == 0 else lax.rem(me + (s - 1), shards)
        if isinstance(s, int) and s == far:
            upper = (count // 2 + 15) // 16 * 16
            first = first + way * upper
            count = count - upper if way else upper
        if not isinstance(first, int):
            first = pl.multiple_of(first, 16)
        ref = buf.at[pl.ds(stream, streams), owner, pl.ds(first, count)]
        turn = (s - 1) % TURNS if isinstance(s, int) else lax.rem(s - 1, TURNS)
        return pltpu.make_async_remote_copy(
            src_ref=ref, dst_ref=ref, send_sem=send_sem.at[lane + way], recv_sem=recv_sem.at[lane + way, turn],
            device_id={"shard": right if way == 0 else left}, device_id_type=MESH,
        )

    def hand(phase, v):
        extra = EXTRA[phase]
        streams = PHASES[phase]
        ref = buf.at[
            pl.ds(streams[0], len(streams)), owner_of(v), pl.ds(pl.multiple_of(odd * (depth - extra), 16), extra)
        ]
        return pltpu.make_async_remote_copy(
            src_ref=ref, dst_ref=ref, send_sem=ysend_sem.at[phase, v], recv_sem=yrecv_sem.at[phase, v],
            device_id={"groups": twin}, device_id_type=MESH,
        )

    def draft_hop(way, s):
        owner = lax.rem(me + shards - (s - 1), shards) if way == 0 else lax.rem(me + (s - 1), shards)
        return pltpu.make_async_remote_copy(
            src_ref=dbuf.at[owner], dst_ref=dbuf.at[owner], send_sem=dsend_sem.at[way],
            recv_sem=drecv_sem.at[way, s - 1], device_id={"shard": right if way == 0 else left}, device_id_type=MESH,
        )

    def launch(phase):
        for piece in pieces(phase):
            for way in range(2):
                hop(piece, way, 1).start()
        if phase == 0:
            for way in range(2):
                draft_hop(way, 1).start()

    def pass_on(phase, s):
        found = pieces(phase)
        owns = sum(piece[-1] for piece in found)
        for k, piece in enumerate(found):
            for way in range(2):
                hop(piece, way, s).wait_recv()
                hop(piece, way, s).wait_send()

                hop(piece, way, s + 1).start()
                if k == owns - 1:
                    hand(phase, 2 * s - 1 + way).start()
        if phase == 0:
            for way in range(2):
                draft_hop(way, s).wait_recv()
                draft_hop(way, s).wait_send()

                if s + 1 < far or way == 0:
                    draft_hop(way, s + 1).start()

    def finish(phase):
        found = pieces(phase)
        owns = sum(piece[-1] for piece in found)
        for k, piece in enumerate(found):
            for way in range(2):
                hop(piece, way, far).wait_recv()
                hop(piece, way, far).wait_send()
            if k == owns - 1:
                hand(phase, 2 * far - 1).start()
        if phase == 0:
            draft_hop(0, far).wait_recv()
            draft_hop(0, far).wait_send()

    def multiply(phase, u):
        streams = PHASES[phase]

        def one(v, _):
            owner = owner_of(v)
            if phase == 0:
                x_load(owner).wait()
                xs[owner, 0:tall] = xin[owner].reshape(tall, depth)
                xs[owner, tall : tall + drafts] = dbuf[owner]

            @pl.when(v > 0)
            def _():
                hand(phase, v).wait_recv()

            w = jnp.concatenate([buf[stream, owner] for stream in streams], 1)
            got = jnp.dot(xs[owner], w, preferred_element_type=F32)
            for k, stream in enumerate(streams):
                acc[stream] += got[:, k * HEAD_DIM : (k + 1) * HEAD_DIM]
            return 0

        lax.fori_loop(2 * u, 2 * u + 2, one, 0)

    def own_rows(count):
        row = lax.rem(lax.broadcasted_iota(jnp.int32, (count, 1), 0), rows)
        pos = row + map_ref[me * per] * BLK
        for j in range(1, per):
            pos = jnp.where(row >= j * BLK, row - j * BLK + map_ref[me * per + j] * BLK, pos)
        return pos

    loads[0].wait()
    loads[1].wait()
    launch(0)

    for stream in range(6):
        acc[stream] = jnp.zeros(acc.shape[1:], F32)
    cosb[...], sinb[...] = rope_tables(own_rows(rows))
    drow = lax.broadcasted_iota(jnp.int32, (drafts, 1), 0)
    dpos = jnp.zeros((drafts, 1), jnp.int32)
    for t in range(steps):
        for b in range(seqs):
            dpos = jnp.where(drow == t * seqs + b, len_ref[b] + t, dpos)
    dcos[...], dsin[...] = rope_tables(dpos)
    seq = lax.broadcasted_iota(jnp.int32, (seqs, rows), 0)
    lengths = jnp.zeros((seqs, rows), jnp.int32)
    for b in range(seqs):
        lengths = jnp.where(seq == b, len_ref[b], lengths)

    def positions(z, _):
        lane = lax.broadcasted_iota(jnp.int32, (seqs, rows), 1)
        where = lane + map_ref[z * per] * BLK
        for j in range(1, per):
            where = jnp.where(lane >= j * BLK, lane - j * BLK + map_ref[z * per + j] * BLK, where)
        kpos[z] = jnp.where(where < lengths, where, FAR)
        return 0

    lax.fori_loop(0, shards, positions, 0)
    limit[0 : G * rows] = jnp.broadcast_to(own_rows(G * rows), (G * rows, HEAD_DIM))
    limit[G * rows : high] = jnp.full((DRAFT_ROWS, HEAD_DIM), FAR - 1, jnp.int32)

    for load in loads[2:]:
        load.wait()

    def own_cache():
        def one(b, _):
            k = acc[0, pl.ds(b, rows, stride=seqs), :]
            v = acc[1, pl.ds(b, rows, stride=seqs), :]
            at = pl.ds(pl.multiple_of(b * rows, rows), rows)
            buf[6, me, at] = rope(k, cosb[...], sinb[...]).astype(BF16)
            buf[7, me, at] = v.astype(BF16)
            return 0

        lax.fori_loop(0, seqs, one, 0)
        dkv[0] = rope(acc[0, tall : tall + drafts, :], dcos[...], dsin[...]).astype(BF16)
        dkv[1] = acc[1, tall : tall + drafts, :].astype(BF16)

    def queries():
        dq = [rope(acc[2 + g, tall : tall + drafts, :], dcos[...], dsin[...]) for g in range(G)]
        for b in range(seqs):
            pieces = [dq[g][t * seqs + b : t * seqs + b + 1] for g in range(G) for t in range(steps)]
            pieces.append(jnp.zeros((DRAFT_ROWS - G * steps, HEAD_DIM), F32))
            qbuf[b, G * rows : high] = jnp.concatenate(pieces, 0).astype(BF16)

        def one(b, _):
            for g in range(G):
                q = acc[2 + g, pl.ds(b, rows, stride=seqs), :]
                qbuf[b, g * rows : (g + 1) * rows] = rope(q, cosb[...], sinb[...]).astype(BF16)
            mbuf[b] = jnp.full((high, HEAD_DIM), NEG, F32)
            lbuf[b] = jnp.zeros((high, HEAD_DIM), F32)
            obuf[b] = jnp.zeros((high, HEAD_DIM), F32)
            return 0

        lax.fori_loop(0, seqs, one, 0)

    def attend(u, tiles=((0, high // 3), (high // 3, high // 3 * 2), (high // 3 * 2, high))):
        first, second = owner_of(2 * u), owner_of(2 * u + 1)

        def one(b, _):
            at = pl.ds(pl.multiple_of(b * rows, rows), rows)
            k = jnp.concatenate([buf[6, first, at, :], buf[6, second, at, :]], 0)
            v = jnp.concatenate([buf[7, first, at, :], buf[7, second, at, :]], 0)
            kp0 = kpos[first, pl.ds(b, 1), :]
            kp1 = kpos[second, pl.ds(b, 1), :]
            for low, end in tiles:
                at_r = slice(low, end)
                s = lax.dot_general(qbuf[b, at_r], k, (((1,), (1,)), ((), ())), preferred_element_type=F32)
                most = limit[at_r]
                s0 = jnp.where(kp0 <= most, s[:, 0:rows], NEG)
                s1 = jnp.where(kp1 <= most, s[:, rows : 2 * rows], NEG)
                before = mbuf[b, at_r]
                top = jnp.maximum(before, jnp.max(jnp.maximum(s0, s1), 1, keepdims=True))
                shrink = jnp.exp2((before - top) * factor)
                w0 = jnp.exp2((s0 - top) * factor)
                w1 = jnp.exp2((s1 - top) * factor)
                mbuf[b, at_r] = top
                lbuf[b, at_r] = lbuf[b, at_r] * shrink + (w0 + w1)
                w = jnp.concatenate([w0, w1], 1).astype(BF16)
                obuf[b, at_r] = obuf[b, at_r] * shrink + jnp.dot(w, v, preferred_element_type=F32)
            return 0

        lax.fori_loop(0, seqs, one, 0)

    for word in ORDER:
        if word == "cache":
            own_cache()
        elif word == "queries":
            queries()
        elif word.startswith("launch"):
            launch("ABC".index(word[-1]))
        elif word[0] == "c":
            attend(int(word[1:]))
        elif word[0] in "ab":
            multiply("ab".index(word[0]), int(word[1:]))
        else:
            phase, s = "ABC".index(word[0]), int(word[1:])
            (finish if s == far else lambda p: pass_on(p, s))(phase)

    attend(far - 1, ((G * rows, high),))
    wo_load.wait()
    r = lax.broadcasted_iota(jnp.int32, (DRAFT_ROWS, drafts), 0)
    c = lax.broadcasted_iota(jnp.int32, (DRAFT_ROWS, drafts), 1)
    for b in range(seqs):
        at_r = slice(G * rows, high)
        new = lax.dot_general(qbuf[b, at_r], dkv[0], (((1,), (1,)), ((), ())), preferred_element_type=F32)
        seen = (lax.rem(c, seqs) == b) & (c // seqs <= lax.rem(r, steps))
        new = jnp.where(seen, new, NEG)
        before = mbuf[b, at_r][:, 0:1]
        top = jnp.maximum(before, jnp.max(new, 1, keepdims=True))
        shrink = jnp.exp2((before - top) * factor)
        w = jnp.where(seen, jnp.exp2((new - top) * factor), 0.0)
        total = jnp.sum(lbuf[b, at_r], 1, keepdims=True) * shrink + jnp.sum(w, 1, keepdims=True)
        mixed = obuf[b, at_r] * shrink + jnp.dot(w.astype(BF16), dkv[1], preferred_element_type=F32)
        attn = (mixed / total).astype(BF16).astype(F32)
        aflat[b * G * steps : (b + 1) * G * steps] = attn[0 : G * steps]
    for g in range(G):
        for t in range(steps):
            lhs[t * seqs : (t + 1) * seqs, g * HEAD_DIM : (g + 1) * HEAD_DIM] = aflat[
                pl.ds(g * steps + t, seqs, stride=G * steps), :
            ]
    partial = jnp.dot(lhs[...].astype(BF16), wo[...], preferred_element_type=F32)
    wide = partial.shape[1] // heads
    for h in range(heads):
        part[h] = partial[:, h * wide : (h + 1) * wide]
    parts[place] = part[head]

    def give(k):
        other = lax.rem(place + k, peers)
        return pltpu.make_async_remote_copy(
            src_ref=part.at[other // pairs], dst_ref=parts.at[place], send_sem=psend_sem.at[k], recv_sem=precv_sem.at[k],
            device_id={"head": other // pairs, "pair": other % pairs}, device_id_type=MESH,
        )

    r1 = lax.broadcasted_iota(jnp.int32, (seqs * G * steps, 1), 0)
    mine = jnp.zeros((seqs * G * steps, 1), jnp.int32)
    for p in range(seqs * G):
        mine = jnp.where(r1 // steps == p, owner_ref[0, p], mine)
    picked = jnp.where(mine == me, aflat[...], 0.0)
    found = [jnp.sum(jnp.where(lax.rem(r1, steps) == t, picked, 0.0), 0, keepdims=True) for t in range(steps)]
    dattn_ref[0, 0] = jnp.concatenate(found, 0).astype(BF16)

    for k in range(1, peers):
        give(k).start()

    attend(far - 1, ((0, 2 * rows), (2 * rows, 4 * rows)))

    def put(b, _):
        for g in range(G):
            at_g = slice(g * rows, (g + 1) * rows)
            total = jnp.sum(lbuf[b, at_g], 1, keepdims=True)
            ostage[g, pl.ds(b, rows, stride=seqs), :] = obuf[b, at_g] / total
        return 0

    lax.fori_loop(0, seqs, put, 0)
    for g in range(G):
        oready[:, :, g * HEAD_DIM : (g + 1) * HEAD_DIM] = ostage[g].astype(BF16).reshape(rows, seqs, HEAD_DIM)
    store = pltpu.make_async_copy(oready, out_hbm, out_sem.at[0])
    store.start()

    for k in range(1, peers):
        give(k).wait_recv()
    summed = jnp.sum(parts[...], 0)
    narrow = wide // pairs
    got = summed[:, 0:narrow]
    for j in range(1, pairs):
        got = jnp.where(pair == j, summed[:, j * narrow : (j + 1) * narrow], got)
    for t in range(steps):
        dec_ref[t] = got[t * seqs : (t + 1) * seqs].astype(BF16)

    for k in range(1, peers):
        give(k).wait_send()

    def drain(v, _):
        for phase in range(2):
            hand(phase, v).wait_send()
        return 0

    lax.fori_loop(1, shards, drain, 0)
    store.wait()


def settle(*refs):
    for k in range(3):
        refs[3 + k][...] = refs[k][...]


def body(groups, shards, heads, pairs, x, d, wq, wk, wv, wo, block_map, prompt_len, owner):
    rows, seqs, width = x.shape
    depth = wq.shape[0]
    steps = d.shape[0]
    drafts = steps * seqs
    tall = rows * seqs
    peers = heads * pairs
    high = G * rows + DRAFT_ROWS
    any_ = pl.BlockSpec(memory_space=pl.ANY)
    vmem = pl.BlockSpec(memory_space=pltpu.VMEM)
    smem = pl.BlockSpec(memory_space=pltpu.SMEM)
    dma = pltpu.SemaphoreType.DMA
    made = pl.pallas_call(
        functools.partial(kernel, groups, shards, heads, pairs),
        out_shape=(
            jax.ShapeDtypeStruct((rows, seqs, wq.shape[1]), BF16),
            jax.ShapeDtypeStruct((1, 1, steps, HEAD_DIM), BF16),
            jax.ShapeDtypeStruct((steps, seqs, wo.shape[1] // peers), BF16),
        ),
        in_specs=[any_, vmem, any_, any_, any_, any_, smem, smem, smem],
        out_specs=(any_, vmem, vmem),
        scratch_shapes=[
            pltpu.VMEM((8, shards, depth, HEAD_DIM), BF16),
            pltpu.VMEM((shards, rows, seqs, depth), BF16),
            pltpu.VMEM((shards, tall + drafts, depth), BF16),
            pltpu.VMEM((shards, drafts, depth), BF16),
            pltpu.VMEM((6, tall + drafts, HEAD_DIM), F32),
            pltpu.VMEM((seqs, high, HEAD_DIM), BF16),
            pltpu.VMEM((seqs, high, HEAD_DIM), F32),
            pltpu.VMEM((seqs, high, HEAD_DIM), F32),
            pltpu.VMEM((seqs, high, HEAD_DIM), F32),
            pltpu.VMEM((high, HEAD_DIM), jnp.int32),
            pltpu.VMEM((G, tall, HEAD_DIM), F32),
            pltpu.VMEM((rows, seqs, wq.shape[1]), BF16),
            pltpu.VMEM((rows, HEAD_DIM), F32),
            pltpu.VMEM((rows, HEAD_DIM), F32),
            pltpu.VMEM((drafts, HEAD_DIM), F32),
            pltpu.VMEM((drafts, HEAD_DIM), F32),
            pltpu.VMEM((shards, seqs, rows), jnp.int32),
            pltpu.VMEM((2, drafts, HEAD_DIM), BF16),
            pltpu.VMEM((seqs * G * steps, HEAD_DIM), F32),
            pltpu.VMEM((drafts, wq.shape[1]), F32),
            pltpu.VMEM(wo.shape, BF16),
            pltpu.VMEM((heads, drafts, wo.shape[1] // heads), F32),
            pltpu.VMEM((peers, drafts, wo.shape[1] // heads), F32),
            dma((7,)),
            dma((shards,)),
            dma((1,)),
            dma((14,)),
            dma((14, TURNS)),
            dma((2, shards)),
            dma((2, shards)),
            dma((2,)),
            dma((2, shards // 2)),
            dma((peers,)),
            dma((peers,)),
        ],
        compiler_params=pltpu.CompilerParams(
            collective_id=0, has_side_effects=True, vmem_limit_bytes=60 * 1024 * 1024
        ),
    )(x, d, wq, wk, wv, wo, block_map, prompt_len, owner)
    prefill, draft, decode = pl.pallas_call(
        settle,
        out_shape=tuple(jax.ShapeDtypeStruct(a.shape, a.dtype) for a in made),
        in_specs=[vmem] * 3,
        out_specs=(vmem,) * 3,
    )(*made)
    return prefill, draft.transpose(2, 0, 1, 3), decode


def solution(mesh):
    placed = (
        P("shard", "groups", None),
        P(None, "groups", "shard"),
        P("shard", ("head", "pair")),
        P("shard", ("head", "pair")),
        P("shard", ("head", "pair")),
        P(("head", "pair"), "shard"),
        P("groups"),
        P("groups"),
        P(("head", "pair"), "groups"),
    )
    sizes = [mesh.shape[name] for name in ("groups", "shard", "head", "pair")]
    return jax.shard_map(
        functools.partial(body, *sizes),
        mesh=mesh,
        in_specs=placed,
        out_specs=(
            P("shard", "groups", ("head", "pair")),
            P(None, ("groups", "shard"), ("head", "pair"), None),
            P(None, "groups", ("shard", "head", "pair")),
        ),
        check_vma=False,
    )
```

```python
import functools
import math

import jax
import jax.numpy as jnp
from jax import lax
from jax.experimental import pallas as pl
from jax.experimental.pallas import tpu as pltpu
from jax.sharding import PartitionSpec as P

HEAD_DIM = 128
G = 4
BLK = 64
NEG = -1e30
THETA = 500000.0
MESH = pl.DeviceIdType.MESH
F32 = jnp.float32
BF16 = jnp.bfloat16
FAR = 1 << 30
DRAFT_ROWS = 16

GROUPS = ((0, 1), (2, 3, 4, 5))
EXTRA = (176, 208)
PARTS = (
    ((0, 1, True), (1, 1, True), (2, 1, True), (0, 1, False), (1, 1, False)),
    ((3, 1, True), (4, 1, True), (5, 1, True), (2, 2, False), (4, 2, False)),
)
HANDS = ((0, 1, 0, 2), (0, 2, 2, 1), (1, 2, 3, 3))
NEEDS = ((0,), (1, 2))
LANES = (0, 10, 0)
TURNS = 4
UNITS_A = {2: (0, 1), 3: (1, 2), 4: (2, 3), 6: (3, 4), 7: (4, 5), 8: (5, 6)}
LATE_A = {1: (6, 7), 3: (7, 8)}
CACHE_AT = 3
UNITS_B = {4: (0, 1), 5: (1, 2), 6: (2, 3), 8: (3, 4)}
LATE_B = {1: (4, 5), 2: (5, 6), 3: (6, 7), 4: (7, 8)}
QUERY_AT = 4
UNITS_C = {4: (0, 1), 5: (1, 3), 6: (3, 5), 7: (5, 7), 8: (7, 8)}


def rope_tables(pos):
    lane = lax.broadcasted_iota(jnp.int32, (pos.shape[0], HEAD_DIM), 1)
    half = HEAD_DIM // 2
    pair = jnp.where(lane < half, lane, lane - half).astype(F32)
    freq = jnp.exp(pair * (-math.log(THETA) / half))
    angle = pos.astype(F32) * freq
    sine = jnp.sin(angle)
    return jnp.cos(angle), jnp.where(lane < half, -sine, sine)


def rope(v, cosine, sine):
    return v * cosine + pltpu.roll(v, HEAD_DIM // 2, 1) * sine


def over(table, s, f):
    low, high = jnp.int32(0), jnp.int32(0)
    for k, (a, b) in table.items():
        low = jnp.where(s == k, a, low)
        high = jnp.where(s == k, b, high)

    def one(u, _):
        f(u)
        return 0

    lax.fori_loop(low, high, one, 0)


def kernel(
    groups, shards, heads, pairs,
    x_hbm, d_ref, wq_hbm, wk_hbm, wv_hbm, wo_hbm, map_ref, len_ref, owner_ref,
    out_hbm, dattn_ref, dec_ref,
    buf, xin, xs, dbuf, acc, qbuf, mbuf, lbuf, obuf, limit, ostage, oready, cosb, sinb, dcos, dsin, kpos,
    dkv, aflat, lhs, wo, part, parts,
    load_sem, x_sem, out_sem, send_sem, recv_sem, ysend_sem, yrecv_sem, dsend_sem, drecv_sem, psend_sem, precv_sem,
):
    me = lax.axis_index("shard")
    head = lax.axis_index("head")
    pair = lax.axis_index("pair")
    group = lax.axis_index("groups")
    right = lax.rem(me + 1, shards)
    left = lax.rem(me + shards - 1, shards)
    odd = lax.rem(group, 2)
    twin = group + 1 - 2 * odd
    far = shards // 2
    rows, seqs, width = x_hbm.shape
    depth = wq_hbm.shape[0]
    steps = d_ref.shape[0]
    tall = rows * seqs
    drafts = steps * seqs
    per = rows // BLK
    scale = 1.0 / math.sqrt(HEAD_DIM)
    factor = scale * math.log2(math.e)
    peers = heads * pairs
    place = head * pairs + pair
    high = G * rows + DRAFT_ROWS

    barrier = pltpu.get_barrier_semaphore()
    for z in (left, right):
        pl.semaphore_signal(barrier, inc=1, device_id={"shard": z}, device_id_type=MESH)
    pl.semaphore_signal(barrier, inc=1, device_id={"groups": twin}, device_id_type=MESH)
    for k in range(1, peers):
        other = lax.rem(place + k, peers)
        pl.semaphore_signal(
            barrier, inc=1, device_id={"head": other // pairs, "pair": other % pairs}, device_id_type=MESH
        )

    def owner_of(v):
        half = (v + 1) // 2
        return lax.rem(me + shards + jnp.where(lax.rem(v, 2) == 1, -half, half), shards)

    sources = [wk_hbm, wv_hbm] + [wq_hbm.at[:, g * HEAD_DIM : (g + 1) * HEAD_DIM] for g in range(G)]
    loads = [pltpu.make_async_copy(src, buf.at[s, me], load_sem.at[s]) for s, src in enumerate(sources)]
    wo_load = pltpu.make_async_copy(wo_hbm, wo, load_sem.at[6])

    def x_load(owner):
        return pltpu.make_async_copy(
            x_hbm.at[:, :, pl.ds(pl.multiple_of(owner * depth, depth), depth)], xin.at[owner], x_sem.at[owner]
        )

    for load in loads:
        load.start()

    def start_x(v, _):
        x_load(owner_of(v)).start()
        return 0

    lax.fori_loop(0, shards, start_x, 0)
    wo_load.start()

    d_all = d_ref[...].astype(F32)
    dbuf[me] = jnp.concatenate([d_all[t] for t in range(steps)], 0).astype(BF16)

    pl.semaphore_wait(barrier, 2 + 1 + peers - 1)

    def pieces(phase):
        if phase == 2:
            found = [(6 + k % 2, 1, k // 2 * (depth // 2), depth // 2) for k in range(4)]
        else:
            found = []
            for stream, count, own in PARTS[phase]:
                extra = EXTRA[0 if stream in GROUPS[0] else 1]
                if own:
                    found.append((stream, count, odd * (depth - extra), extra))
                else:
                    found.append((stream, count, extra, depth - 2 * extra))
        return [(LANES[phase] + 2 * k, *piece) for k, piece in enumerate(found)]

    def hop(piece, way, s):
        lane, stream, streams, first, count = piece
        owner = lax.rem(me + shards - (s - 1), shards) if way == 0 else lax.rem(me + (s - 1), shards)
        if isinstance(s, int) and s == far:
            upper = (count // 2 + 15) // 16 * 16
            first = first + way * upper
            count = count - upper if way else upper
        if not isinstance(first, int):
            first = pl.multiple_of(first, 16)
        ref = buf.at[pl.ds(stream, streams), owner, pl.ds(first, count)]
        turn = (s - 1) % TURNS if isinstance(s, int) else lax.rem(s - 1, TURNS)
        return pltpu.make_async_remote_copy(
            src_ref=ref, dst_ref=ref, send_sem=send_sem.at[lane + way], recv_sem=recv_sem.at[lane + way, turn],
            device_id={"shard": right if way == 0 else left}, device_id_type=MESH,
        )

    def hand(k, v):
        _, _, stream, streams = HANDS[k]
        extra = EXTRA[0 if stream in GROUPS[0] else 1]
        ref = buf.at[
            pl.ds(stream, streams), owner_of(v), pl.ds(pl.multiple_of(odd * (depth - extra), 16), extra)
        ]
        return pltpu.make_async_remote_copy(
            src_ref=ref, dst_ref=ref, send_sem=ysend_sem.at[k, v], recv_sem=yrecv_sem.at[k, v],
            device_id={"groups": twin}, device_id_type=MESH,
        )

    def hands(phase, part, v):
        for k, (at, after, _, _) in enumerate(HANDS):
            if at == phase and after == part:
                hand(k, v).start()

    def draft_hop(way, s):
        owner = lax.rem(me + shards - (s - 1), shards) if way == 0 else lax.rem(me + (s - 1), shards)
        return pltpu.make_async_remote_copy(
            src_ref=dbuf.at[owner], dst_ref=dbuf.at[owner], send_sem=dsend_sem.at[way],
            recv_sem=drecv_sem.at[way, s - 1], device_id={"shard": right if way == 0 else left}, device_id_type=MESH,
        )

    def launch(phase):
        for piece in pieces(phase):
            for way in range(2):
                hop(piece, way, 1).start()
        if phase == 0:
            for way in range(2):
                draft_hop(way, 1).start()

    def pass_on(phase, s):
        for k, piece in enumerate(pieces(phase)):
            for way in range(2):
                hop(piece, way, s).wait_recv()
                hop(piece, way, s).wait_send()

                @pl.when(s < far - 1)
                def _():
                    hop(piece, way, s + 1).start()

                @pl.when(s == far - 1)
                def _():
                    hop(piece, way, far).start()

                hands(phase, k, 2 * s - 1 + way)
        if phase == 0:
            for way in range(2):
                draft_hop(way, s).wait_recv()
                draft_hop(way, s).wait_send()

            draft_hop(0, s + 1).start()

            @pl.when(s < far - 1)
            def _():
                draft_hop(1, s + 1).start()

        if phase < 2:

            @pl.when(s == far - 1)
            def _():
                launch(phase + 1)

    def finish(phase):
        for k, piece in enumerate(pieces(phase)):
            for way in range(2):
                hop(piece, way, far).wait_recv()
                hop(piece, way, far).wait_send()
            hands(phase, k, 2 * far - 1)
        if phase == 0:
            draft_hop(0, far).wait_recv()
            draft_hop(0, far).wait_send()

    def ring(phase, work):
        def step(s, _):
            @pl.when(s < far)
            def _():
                pass_on(phase, s)

            @pl.when(s == far)
            def _():
                finish(phase)

            work(s)
            return 0

        lax.fori_loop(1, far + 1, step, 0)

    def multiply(phase, u):
        streams = GROUPS[phase]

        def one(v, _):
            owner = owner_of(v)
            if phase == 0:
                x_load(owner).wait()
                xs[owner, 0:tall] = xin[owner].reshape(tall, depth)
                xs[owner, tall : tall + drafts] = dbuf[owner]

            @pl.when(v > 0)
            def _():
                for k in NEEDS[phase]:
                    hand(k, v).wait_recv()

            w = jnp.concatenate([buf[stream, owner] for stream in streams], 1)
            got = jnp.dot(xs[owner], w, preferred_element_type=F32)
            for k, stream in enumerate(streams):
                acc[stream] += got[:, k * HEAD_DIM : (k + 1) * HEAD_DIM]
            return 0

        lax.fori_loop(2 * u, 2 * u + 2, one, 0)

    def own_rows(count):
        row = lax.rem(lax.broadcasted_iota(jnp.int32, (count, 1), 0), rows)
        pos = row + map_ref[me * per] * BLK
        for j in range(1, per):
            pos = jnp.where(row >= j * BLK, row - j * BLK + map_ref[me * per + j] * BLK, pos)
        return pos

    for load in loads[:3]:
        load.wait()
    launch(0)

    for stream in range(6):
        acc[stream] = jnp.zeros(acc.shape[1:], F32)
    cosb[...], sinb[...] = rope_tables(own_rows(rows))
    drow = lax.broadcasted_iota(jnp.int32, (drafts, 1), 0)
    dpos = jnp.zeros((drafts, 1), jnp.int32)
    for t in range(steps):
        for b in range(seqs):
            dpos = jnp.where(drow == t * seqs + b, len_ref[b] + t, dpos)
    dcos[...], dsin[...] = rope_tables(dpos)
    seq = lax.broadcasted_iota(jnp.int32, (seqs, rows), 0)
    lengths = jnp.zeros((seqs, rows), jnp.int32)
    for b in range(seqs):
        lengths = jnp.where(seq == b, len_ref[b], lengths)

    def positions(z, _):
        lane = lax.broadcasted_iota(jnp.int32, (seqs, rows), 1)
        where = lane + map_ref[z * per] * BLK
        for j in range(1, per):
            where = jnp.where(lane >= j * BLK, lane - j * BLK + map_ref[z * per + j] * BLK, where)
        kpos[z] = jnp.where(where < lengths, where, FAR)
        return 0

    lax.fori_loop(0, shards, positions, 0)
    limit[0 : G * rows] = jnp.broadcast_to(own_rows(G * rows), (G * rows, HEAD_DIM))
    limit[G * rows : high] = jnp.full((DRAFT_ROWS, HEAD_DIM), FAR - 1, jnp.int32)

    for load in loads[3:]:
        load.wait()
    ring(0, lambda s: over(UNITS_A, s, functools.partial(multiply, 0)))

    def own_cache():
        def one(b, _):
            k = acc[0, pl.ds(b, rows, stride=seqs), :]
            v = acc[1, pl.ds(b, rows, stride=seqs), :]
            at = pl.ds(pl.multiple_of(b * rows, rows), rows)
            buf[6, me, at] = rope(k, cosb[...], sinb[...]).astype(BF16)
            buf[7, me, at] = v.astype(BF16)
            return 0

        lax.fori_loop(0, seqs, one, 0)
        dkv[0] = rope(acc[0, tall : tall + drafts, :], dcos[...], dsin[...]).astype(BF16)
        dkv[1] = acc[1, tall : tall + drafts, :].astype(BF16)

    def work1(s):
        over(LATE_A, s, functools.partial(multiply, 0))
        pl.when(s == CACHE_AT)(own_cache)
        over(UNITS_B, s, functools.partial(multiply, 1))

    ring(1, work1)

    def queries():
        dq = [rope(acc[2 + g, tall : tall + drafts, :], dcos[...], dsin[...]) for g in range(G)]
        for b in range(seqs):
            pieces = [dq[g][t * seqs + b : t * seqs + b + 1] for g in range(G) for t in range(steps)]
            pieces.append(jnp.zeros((DRAFT_ROWS - G * steps, HEAD_DIM), F32))
            qbuf[b, G * rows : high] = jnp.concatenate(pieces, 0).astype(BF16)

        def one(b, _):
            for g in range(G):
                q = acc[2 + g, pl.ds(b, rows, stride=seqs), :]
                qbuf[b, g * rows : (g + 1) * rows] = rope(q, cosb[...], sinb[...]).astype(BF16)
            mbuf[b] = jnp.full((high, HEAD_DIM), NEG, F32)
            lbuf[b] = jnp.zeros((high, HEAD_DIM), F32)
            obuf[b] = jnp.zeros((high, HEAD_DIM), F32)
            return 0

        lax.fori_loop(0, seqs, one, 0)

    def attend(u, tiles=((0, high // 3), (high // 3, high // 3 * 2), (high // 3 * 2, high))):
        first, second = owner_of(2 * u), owner_of(2 * u + 1)

        def one(b, _):
            at = pl.ds(pl.multiple_of(b * rows, rows), rows)
            k = jnp.concatenate([buf[6, first, at, :], buf[6, second, at, :]], 0)
            v = jnp.concatenate([buf[7, first, at, :], buf[7, second, at, :]], 0)
            kp0 = kpos[first, pl.ds(b, 1), :]
            kp1 = kpos[second, pl.ds(b, 1), :]
            for low, end in tiles:
                at_r = slice(low, end)
                s = lax.dot_general(qbuf[b, at_r], k, (((1,), (1,)), ((), ())), preferred_element_type=F32)
                most = limit[at_r]
                s0 = jnp.where(kp0 <= most, s[:, 0:rows], NEG)
                s1 = jnp.where(kp1 <= most, s[:, rows : 2 * rows], NEG)
                before = mbuf[b, at_r]
                top = jnp.maximum(before, jnp.max(jnp.maximum(s0, s1), 1, keepdims=True))
                shrink = jnp.exp2((before - top) * factor)
                w0 = jnp.exp2((s0 - top) * factor)
                w1 = jnp.exp2((s1 - top) * factor)
                mbuf[b, at_r] = top
                lbuf[b, at_r] = lbuf[b, at_r] * shrink + (w0 + w1)
                w = jnp.concatenate([w0, w1], 1).astype(BF16)
                obuf[b, at_r] = obuf[b, at_r] * shrink + jnp.dot(w, v, preferred_element_type=F32)
            return 0

        lax.fori_loop(0, seqs, one, 0)

    wide = wo.shape[1] // heads

    def give(k):
        other = lax.rem(place + k, peers)
        return pltpu.make_async_remote_copy(
            src_ref=part.at[other // pairs], dst_ref=parts.at[place], send_sem=psend_sem.at[k], recv_sem=precv_sem.at[k],
            device_id={"head": other // pairs, "pair": other % pairs}, device_id_type=MESH,
        )

    def draft_outputs():
        attend(far - 1, ((G * rows, high),))
        wo_load.wait()
        r = lax.broadcasted_iota(jnp.int32, (DRAFT_ROWS, drafts), 0)
        c = lax.broadcasted_iota(jnp.int32, (DRAFT_ROWS, drafts), 1)
        for b in range(seqs):
            at_r = slice(G * rows, high)
            new = lax.dot_general(qbuf[b, at_r], dkv[0], (((1,), (1,)), ((), ())), preferred_element_type=F32)
            seen = (lax.rem(c, seqs) == b) & (c // seqs <= lax.rem(r, steps))
            new = jnp.where(seen, new, NEG)
            before = mbuf[b, at_r][:, 0:1]
            top = jnp.maximum(before, jnp.max(new, 1, keepdims=True))
            shrink = jnp.exp2((before - top) * factor)
            w = jnp.where(seen, jnp.exp2((new - top) * factor), 0.0)
            total = jnp.sum(lbuf[b, at_r], 1, keepdims=True) * shrink + jnp.sum(w, 1, keepdims=True)
            mixed = obuf[b, at_r] * shrink + jnp.dot(w.astype(BF16), dkv[1], preferred_element_type=F32)
            attn = (mixed / total).astype(BF16).astype(F32)
            aflat[b * G * steps : (b + 1) * G * steps] = attn[0 : G * steps]
        for g in range(G):
            for t in range(steps):
                lhs[t * seqs : (t + 1) * seqs, g * HEAD_DIM : (g + 1) * HEAD_DIM] = aflat[
                    pl.ds(g * steps + t, seqs, stride=G * steps), :
                ]
        partial = jnp.dot(lhs[...].astype(BF16), wo[...], preferred_element_type=F32)
        for h in range(heads):
            part[h] = partial[:, h * wide : (h + 1) * wide]
        parts[place] = part[head]

        r1 = lax.broadcasted_iota(jnp.int32, (seqs * G * steps, 1), 0)
        mine = jnp.zeros((seqs * G * steps, 1), jnp.int32)
        for p in range(seqs * G):
            mine = jnp.where(r1 // steps == p, owner_ref[0, p], mine)
        picked = jnp.where(mine == me, aflat[...], 0.0)
        found = [jnp.sum(jnp.where(lax.rem(r1, steps) == t, picked, 0.0), 0, keepdims=True) for t in range(steps)]
        dattn_ref[0, 0] = jnp.concatenate(found, 0).astype(BF16)

        for k in range(1, peers):
            give(k).start()

    def work2(s):
        over(LATE_B, s, functools.partial(multiply, 1))
        pl.when(s == QUERY_AT)(queries)
        pl.when(s == far)(draft_outputs)
        over(UNITS_C, s, attend)

    ring(2, work2)

    def put(b, _):
        for g in range(G):
            at_g = slice(g * rows, (g + 1) * rows)
            total = jnp.sum(lbuf[b, at_g], 1, keepdims=True)
            ostage[g, pl.ds(b, rows, stride=seqs), :] = obuf[b, at_g] / total
        return 0

    lax.fori_loop(0, seqs, put, 0)
    for g in range(G):
        oready[:, :, g * HEAD_DIM : (g + 1) * HEAD_DIM] = ostage[g].astype(BF16).reshape(rows, seqs, HEAD_DIM)
    store = pltpu.make_async_copy(oready, out_hbm, out_sem.at[0])
    store.start()

    for k in range(1, peers):
        give(k).wait_recv()
    summed = jnp.sum(parts[...], 0)
    narrow = wide // pairs
    got = summed[:, 0:narrow]
    for j in range(1, pairs):
        got = jnp.where(pair == j, summed[:, j * narrow : (j + 1) * narrow], got)
    for t in range(steps):
        dec_ref[t] = got[t * seqs : (t + 1) * seqs].astype(BF16)

    for k in range(1, peers):
        give(k).wait_send()

    def drain(v, _):
        for k in range(len(HANDS)):
            hand(k, v).wait_send()
        return 0

    lax.fori_loop(1, shards, drain, 0)
    store.wait()


def settle(*refs):
    for k in range(3):
        refs[3 + k][...] = refs[k][...]


def body(groups, shards, heads, pairs, x, d, wq, wk, wv, wo, block_map, prompt_len, owner):
    rows, seqs, width = x.shape
    depth = wq.shape[0]
    steps = d.shape[0]
    drafts = steps * seqs
    tall = rows * seqs
    peers = heads * pairs
    high = G * rows + DRAFT_ROWS
    any_ = pl.BlockSpec(memory_space=pl.ANY)
    vmem = pl.BlockSpec(memory_space=pltpu.VMEM)
    smem = pl.BlockSpec(memory_space=pltpu.SMEM)
    dma = pltpu.SemaphoreType.DMA
    made = pl.pallas_call(
        functools.partial(kernel, groups, shards, heads, pairs),
        out_shape=(
            jax.ShapeDtypeStruct((rows, seqs, wq.shape[1]), BF16),
            jax.ShapeDtypeStruct((1, 1, steps, HEAD_DIM), BF16),
            jax.ShapeDtypeStruct((steps, seqs, wo.shape[1] // peers), BF16),
        ),
        in_specs=[any_, vmem, any_, any_, any_, any_, smem, smem, smem],
        out_specs=(any_, vmem, vmem),
        scratch_shapes=[
            pltpu.VMEM((8, shards, depth, HEAD_DIM), BF16),
            pltpu.VMEM((shards, rows, seqs, depth), BF16),
            pltpu.VMEM((shards, tall + drafts, depth), BF16),
            pltpu.VMEM((shards, drafts, depth), BF16),
            pltpu.VMEM((6, tall + drafts, HEAD_DIM), F32),
            pltpu.VMEM((seqs, high, HEAD_DIM), BF16),
            pltpu.VMEM((seqs, high, HEAD_DIM), F32),
            pltpu.VMEM((seqs, high, HEAD_DIM), F32),
            pltpu.VMEM((seqs, high, HEAD_DIM), F32),
            pltpu.VMEM((high, HEAD_DIM), jnp.int32),
            pltpu.VMEM((G, tall, HEAD_DIM), F32),
            pltpu.VMEM((rows, seqs, wq.shape[1]), BF16),
            pltpu.VMEM((rows, HEAD_DIM), F32),
            pltpu.VMEM((rows, HEAD_DIM), F32),
            pltpu.VMEM((drafts, HEAD_DIM), F32),
            pltpu.VMEM((drafts, HEAD_DIM), F32),
            pltpu.VMEM((shards, seqs, rows), jnp.int32),
            pltpu.VMEM((2, drafts, HEAD_DIM), BF16),
            pltpu.VMEM((seqs * G * steps, HEAD_DIM), F32),
            pltpu.VMEM((drafts, wq.shape[1]), F32),
            pltpu.VMEM(wo.shape, BF16),
            pltpu.VMEM((heads, drafts, wo.shape[1] // heads), F32),
            pltpu.VMEM((peers, drafts, wo.shape[1] // heads), F32),
            dma((7,)),
            dma((shards,)),
            dma((1,)),
            dma((20,)),
            dma((20, TURNS)),
            dma((len(HANDS), shards)),
            dma((len(HANDS), shards)),
            dma((2,)),
            dma((2, shards // 2)),
            dma((peers,)),
            dma((peers,)),
        ],
        compiler_params=pltpu.CompilerParams(
            collective_id=0, has_side_effects=True, vmem_limit_bytes=60 * 1024 * 1024
        ),
    )(x, d, wq, wk, wv, wo, block_map, prompt_len, owner)
    prefill, draft, decode = pl.pallas_call(
        settle,
        out_shape=tuple(jax.ShapeDtypeStruct(a.shape, a.dtype) for a in made),
        in_specs=[vmem] * 3,
        out_specs=(vmem,) * 3,
    )(*made)
    return prefill, draft.transpose(2, 0, 1, 3), decode


def solution(mesh):
    placed = (
        P("shard", "groups", None),
        P(None, "groups", "shard"),
        P("shard", ("head", "pair")),
        P("shard", ("head", "pair")),
        P("shard", ("head", "pair")),
        P(("head", "pair"), "shard"),
        P("groups"),
        P("groups"),
        P(("head", "pair"), "groups"),
    )
    sizes = [mesh.shape[name] for name in ("groups", "shard", "head", "pair")]
    return jax.shard_map(
        functools.partial(body, *sizes),
        mesh=mesh,
        in_specs=placed,
        out_specs=(
            P("shard", "groups", ("head", "pair")),
            P(None, ("groups", "shard"), ("head", "pair"), None),
            P(None, "groups", ("shard", "head", "pair")),
        ),
        check_vma=False,
    )
```

```python
import functools
import math

import jax
import jax.numpy as jnp
from jax import lax
from jax.experimental import pallas as pl
from jax.experimental.pallas import tpu as pltpu
from jax.sharding import PartitionSpec as P

HEAD_DIM = 128
G = 4
BLK = 64
NEG = -1e30
THETA = 500000.0
MESH = pl.DeviceIdType.MESH
F32 = jnp.float32
BF16 = jnp.bfloat16
FAR = 1 << 30
DRAFT_ROWS = 16

GROUPS = ((0, 1), (2,), (3, 4, 5))
EXTRA = (176, 208)
PARTS = (
    ((0, 1, True), (1, 1, True), (2, 1, True), (0, 1, False), (1, 1, False)),
    ((3, 1, True), (4, 1, True), (5, 1, True), (2, 2, False), (4, 2, False)),
)
HANDS = ((0, 1, 0, 2), (0, 2, 2, 1), (1, 2, 3, 3))
NEEDS = ((0,), (1,), (2,))
LANES = (0, 10, 0)
TURNS = 4
UNITS_A = {2: (0, 1), 3: (1, 2), 4: (2, 3), 6: (3, 4), 7: (4, 5), 8: (5, 6)}
LATE_A = {1: (6, 7), 3: (7, 8)}
CACHE_AT = 3
UNITS_B = {4: (0, 1), 5: (1, 2), 6: (2, 3), 8: (3, 4)}
LATE_B = {1: (4, 5), 2: (5, 6), 3: (6, 7), 4: (7, 8)}
QUERY_AT = 4
UNITS_C = {4: (0, 2), 5: (2, 4), 6: (4, 6), 7: (6, 7), 8: (7, 8)}
UNITS_HEAD = {s: (s - 1, s) for s in range(1, 9)}


def rope_tables(pos):
    lane = lax.broadcasted_iota(jnp.int32, (pos.shape[0], HEAD_DIM), 1)
    half = HEAD_DIM // 2
    pair = jnp.where(lane < half, lane, lane - half).astype(F32)
    freq = jnp.exp(pair * (-math.log(THETA) / half))
    angle = pos.astype(F32) * freq
    sine = jnp.sin(angle)
    return jnp.cos(angle), jnp.where(lane < half, -sine, sine)


def rope(v, cosine, sine):
    return v * cosine + pltpu.roll(v, HEAD_DIM // 2, 1) * sine


def over(table, s, f):
    low, high = jnp.int32(0), jnp.int32(0)
    for k, (a, b) in table.items():
        low = jnp.where(s == k, a, low)
        high = jnp.where(s == k, b, high)

    def one(u, _):
        f(u)
        return 0

    lax.fori_loop(low, high, one, 0)


def kernel(
    groups, shards, heads, pairs,
    x_hbm, d_ref, wq_hbm, wk_hbm, wv_hbm, wo_hbm, map_ref, len_ref, owner_ref,
    out_hbm, dattn_ref, dec_ref,
    buf, xin, xs, dbuf, acc, qbuf, mbuf, lbuf, obuf, limit, ostage, oready, cosb, sinb, dcos, dsin, kpos,
    dkv, aflat, lhs, wo, part, parts,
    load_sem, x_sem, out_sem, send_sem, recv_sem, ysend_sem, yrecv_sem, dsend_sem, drecv_sem, psend_sem, precv_sem,
):
    me = lax.axis_index("shard")
    head = lax.axis_index("head")
    pair = lax.axis_index("pair")
    group = lax.axis_index("groups")
    right = lax.rem(me + 1, shards)
    left = lax.rem(me + shards - 1, shards)
    odd = lax.rem(group, 2)
    twin = group + 1 - 2 * odd
    far = shards // 2
    rows, seqs, width = x_hbm.shape
    depth = wq_hbm.shape[0]
    steps = d_ref.shape[0]
    tall = rows * seqs
    drafts = steps * seqs
    per = rows // BLK
    scale = 1.0 / math.sqrt(HEAD_DIM)
    factor = scale * math.log2(math.e)
    peers = heads * pairs
    place = head * pairs + pair
    high = G * rows + DRAFT_ROWS

    barrier = pltpu.get_barrier_semaphore()
    for z in (left, right):
        pl.semaphore_signal(barrier, inc=1, device_id={"shard": z}, device_id_type=MESH)
    pl.semaphore_signal(barrier, inc=1, device_id={"groups": twin}, device_id_type=MESH)
    for k in range(1, peers):
        other = lax.rem(place + k, peers)
        pl.semaphore_signal(
            barrier, inc=1, device_id={"head": other // pairs, "pair": other % pairs}, device_id_type=MESH
        )

    def owner_of(v):
        half = (v + 1) // 2
        return lax.rem(me + shards + jnp.where(lax.rem(v, 2) == 1, -half, half), shards)

    sources = [wk_hbm, wv_hbm] + [wq_hbm.at[:, g * HEAD_DIM : (g + 1) * HEAD_DIM] for g in range(G)]
    loads = [pltpu.make_async_copy(src, buf.at[s, me], load_sem.at[s]) for s, src in enumerate(sources)]
    wo_load = pltpu.make_async_copy(wo_hbm, wo, load_sem.at[6])

    def x_load(owner):
        return pltpu.make_async_copy(
            x_hbm.at[:, :, pl.ds(pl.multiple_of(owner * depth, depth), depth)], xin.at[owner], x_sem.at[owner]
        )

    for load in loads:
        load.start()

    def start_x(v, _):
        x_load(owner_of(v)).start()
        return 0

    lax.fori_loop(0, shards, start_x, 0)
    wo_load.start()

    d_all = d_ref[...].astype(F32)
    dbuf[me] = jnp.concatenate([d_all[t] for t in range(steps)], 0).astype(BF16)

    pl.semaphore_wait(barrier, 2 + 1 + peers - 1)

    def pieces(phase):
        if phase == 2:
            found = [(6 + k % 2, 1, k // 2 * (depth // 2), depth // 2) for k in range(4)]
        else:
            found = []
            for stream, count, own in PARTS[phase]:
                extra = EXTRA[0 if stream in GROUPS[0] else 1]
                if own:
                    found.append((stream, count, odd * (depth - extra), extra))
                else:
                    found.append((stream, count, extra, depth - 2 * extra))
        return [(LANES[phase] + 2 * k, *piece) for k, piece in enumerate(found)]

    def hop(piece, way, s):
        lane, stream, streams, first, count = piece
        owner = lax.rem(me + shards - (s - 1), shards) if way == 0 else lax.rem(me + (s - 1), shards)
        if isinstance(s, int) and s == far:
            upper = (count // 2 + 15) // 16 * 16
            first = first + way * upper
            count = count - upper if way else upper
        if not isinstance(first, int):
            first = pl.multiple_of(first, 16)
        ref = buf.at[pl.ds(stream, streams), owner, pl.ds(first, count)]
        turn = (s - 1) % TURNS if isinstance(s, int) else lax.rem(s - 1, TURNS)
        return pltpu.make_async_remote_copy(
            src_ref=ref, dst_ref=ref, send_sem=send_sem.at[lane + way], recv_sem=recv_sem.at[lane + way, turn],
            device_id={"shard": right if way == 0 else left}, device_id_type=MESH,
        )

    def hand(k, v):
        _, _, stream, streams = HANDS[k]
        extra = EXTRA[0 if stream in GROUPS[0] else 1]
        ref = buf.at[
            pl.ds(stream, streams), owner_of(v), pl.ds(pl.multiple_of(odd * (depth - extra), 16), extra)
        ]
        return pltpu.make_async_remote_copy(
            src_ref=ref, dst_ref=ref, send_sem=ysend_sem.at[k, v], recv_sem=yrecv_sem.at[k, v],
            device_id={"groups": twin}, device_id_type=MESH,
        )

    def hands(phase, part, v):
        for k, (at, after, _, _) in enumerate(HANDS):
            if at == phase and after == part:
                hand(k, v).start()

    def draft_hop(way, s):
        owner = lax.rem(me + shards - (s - 1), shards) if way == 0 else lax.rem(me + (s - 1), shards)
        return pltpu.make_async_remote_copy(
            src_ref=dbuf.at[owner], dst_ref=dbuf.at[owner], send_sem=dsend_sem.at[way],
            recv_sem=drecv_sem.at[way, s - 1], device_id={"shard": right if way == 0 else left}, device_id_type=MESH,
        )

    def launch(phase):
        for piece in pieces(phase):
            for way in range(2):
                hop(piece, way, 1).start()
        if phase == 0:
            for way in range(2):
                draft_hop(way, 1).start()

    def pass_on(phase, s):
        for k, piece in enumerate(pieces(phase)):
            for way in range(2):
                hop(piece, way, s).wait_recv()
                hop(piece, way, s).wait_send()

                @pl.when(s < far - 1)
                def _():
                    hop(piece, way, s + 1).start()

                @pl.when(s == far - 1)
                def _():
                    hop(piece, way, far).start()

                hands(phase, k, 2 * s - 1 + way)
        if phase == 0:
            for way in range(2):
                draft_hop(way, s).wait_recv()
                draft_hop(way, s).wait_send()

            draft_hop(0, s + 1).start()

            @pl.when(s < far - 1)
            def _():
                draft_hop(1, s + 1).start()

        if phase < 2:

            @pl.when(s == far - 1)
            def _():
                launch(phase + 1)

    def finish(phase):
        for k, piece in enumerate(pieces(phase)):
            for way in range(2):
                hop(piece, way, far).wait_recv()
                hop(piece, way, far).wait_send()
            hands(phase, k, 2 * far - 1)
        if phase == 0:
            draft_hop(0, far).wait_recv()
            draft_hop(0, far).wait_send()

    def ring(phase, work):
        def step(s, _):
            @pl.when(s < far)
            def _():
                pass_on(phase, s)

            @pl.when(s == far)
            def _():
                finish(phase)

            work(s)
            return 0

        lax.fori_loop(1, far + 1, step, 0)

    def multiply(group_at, u):
        streams = GROUPS[group_at]

        def one(v, _):
            owner = owner_of(v)
            if group_at == 0:
                x_load(owner).wait()
                xs[owner, 0:tall] = xin[owner].reshape(tall, depth)
                xs[owner, tall : tall + drafts] = dbuf[owner]

            @pl.when(v > 0)
            def _():
                for k in NEEDS[group_at]:
                    hand(k, v).wait_recv()

            w = jnp.concatenate([buf[stream, owner] for stream in streams], 1)
            got = jnp.dot(xs[owner], w, preferred_element_type=F32)
            for k, stream in enumerate(streams):
                acc[stream] += got[:, k * HEAD_DIM : (k + 1) * HEAD_DIM]
            return 0

        lax.fori_loop(2 * u, 2 * u + 2, one, 0)

    def own_rows(count):
        row = lax.rem(lax.broadcasted_iota(jnp.int32, (count, 1), 0), rows)
        pos = row + map_ref[me * per] * BLK
        for j in range(1, per):
            pos = jnp.where(row >= j * BLK, row - j * BLK + map_ref[me * per + j] * BLK, pos)
        return pos

    for load in loads[:3]:
        load.wait()
    launch(0)

    for stream in range(6):
        acc[stream] = jnp.zeros(acc.shape[1:], F32)
    cosb[...], sinb[...] = rope_tables(own_rows(rows))
    drow = lax.broadcasted_iota(jnp.int32, (drafts, 1), 0)
    dpos = jnp.zeros((drafts, 1), jnp.int32)
    for t in range(steps):
        for b in range(seqs):
            dpos = jnp.where(drow == t * seqs + b, len_ref[b] + t, dpos)
    dcos[...], dsin[...] = rope_tables(dpos)
    seq = lax.broadcasted_iota(jnp.int32, (seqs, rows), 0)
    lengths = jnp.zeros((seqs, rows), jnp.int32)
    for b in range(seqs):
        lengths = jnp.where(seq == b, len_ref[b], lengths)

    def positions(z, _):
        lane = lax.broadcasted_iota(jnp.int32, (seqs, rows), 1)
        where = lane + map_ref[z * per] * BLK
        for j in range(1, per):
            where = jnp.where(lane >= j * BLK, lane - j * BLK + map_ref[z * per + j] * BLK, where)
        kpos[z] = jnp.where(where < lengths, where, FAR)
        return 0

    lax.fori_loop(0, shards, positions, 0)
    limit[0 : G * rows] = jnp.broadcast_to(own_rows(G * rows), (G * rows, HEAD_DIM))
    limit[G * rows : high] = jnp.full((DRAFT_ROWS, HEAD_DIM), FAR - 1, jnp.int32)

    for load in loads[3:]:
        load.wait()
    ring(0, lambda s: over(UNITS_A, s, functools.partial(multiply, 0)))

    def own_cache():
        def one(b, _):
            k = acc[0, pl.ds(b, rows, stride=seqs), :]
            v = acc[1, pl.ds(b, rows, stride=seqs), :]
            at = pl.ds(pl.multiple_of(b * rows, rows), rows)
            buf[6, me, at] = rope(k, cosb[...], sinb[...]).astype(BF16)
            buf[7, me, at] = v.astype(BF16)
            return 0

        lax.fori_loop(0, seqs, one, 0)
        dkv[0] = rope(acc[0, tall : tall + drafts, :], dcos[...], dsin[...]).astype(BF16)
        dkv[1] = acc[1, tall : tall + drafts, :].astype(BF16)

    def work1(s):
        over(LATE_A, s, functools.partial(multiply, 0))
        pl.when(s == CACHE_AT)(own_cache)
        over(UNITS_HEAD, s, functools.partial(multiply, 1))
        over(UNITS_B, s, functools.partial(multiply, 2))

    ring(1, work1)

    def rotated(b, g):
        q = acc[2 + g, pl.ds(b, rows, stride=seqs), :]
        qbuf[b, g * rows : (g + 1) * rows] = rope(q, cosb[...], sinb[...]).astype(BF16)

    def first_queries():
        def one(b, _):
            rotated(b, 0)
            mbuf[b] = jnp.full((high, HEAD_DIM), NEG, F32)
            lbuf[b] = jnp.zeros((high, HEAD_DIM), F32)
            obuf[b] = jnp.zeros((high, HEAD_DIM), F32)
            return 0

        lax.fori_loop(0, seqs, one, 0)

    def queries():
        dq = [rope(acc[2 + g, tall : tall + drafts, :], dcos[...], dsin[...]) for g in range(G)]
        for b in range(seqs):
            pieces = [dq[g][t * seqs + b : t * seqs + b + 1] for g in range(G) for t in range(steps)]
            pieces.append(jnp.zeros((DRAFT_ROWS - G * steps, HEAD_DIM), F32))
            qbuf[b, G * rows : high] = jnp.concatenate(pieces, 0).astype(BF16)

        def one(b, _):
            for g in range(1, G):
                rotated(b, g)
            return 0

        lax.fori_loop(0, seqs, one, 0)

    middle = rows + (high - rows) // 32 * 16
    rest = ((rows, middle), (middle, high))

    def attend(u, tiles=rest):
        first, second = owner_of(2 * u), owner_of(2 * u + 1)

        def one(b, _):
            at = pl.ds(pl.multiple_of(b * rows, rows), rows)
            k = jnp.concatenate([buf[6, first, at, :], buf[6, second, at, :]], 0)
            v = jnp.concatenate([buf[7, first, at, :], buf[7, second, at, :]], 0)
            kp0 = kpos[first, pl.ds(b, 1), :]
            kp1 = kpos[second, pl.ds(b, 1), :]
            for low, end in tiles:
                at_r = slice(low, end)
                s = lax.dot_general(qbuf[b, at_r], k, (((1,), (1,)), ((), ())), preferred_element_type=F32)
                most = limit[at_r]
                s0 = jnp.where(kp0 <= most, s[:, 0:rows], NEG)
                s1 = jnp.where(kp1 <= most, s[:, rows : 2 * rows], NEG)
                before = mbuf[b, at_r]
                top = jnp.maximum(before, jnp.max(jnp.maximum(s0, s1), 1, keepdims=True))
                shrink = jnp.exp2((before - top) * factor)
                w0 = jnp.exp2((s0 - top) * factor)
                w1 = jnp.exp2((s1 - top) * factor)
                mbuf[b, at_r] = top
                lbuf[b, at_r] = lbuf[b, at_r] * shrink + (w0 + w1)
                w = jnp.concatenate([w0, w1], 1).astype(BF16)
                obuf[b, at_r] = obuf[b, at_r] * shrink + jnp.dot(w, v, preferred_element_type=F32)
            return 0

        lax.fori_loop(0, seqs, one, 0)

    wide = wo.shape[1] // heads

    def give(k):
        other = lax.rem(place + k, peers)
        return pltpu.make_async_remote_copy(
            src_ref=part.at[other // pairs], dst_ref=parts.at[place], send_sem=psend_sem.at[k], recv_sem=precv_sem.at[k],
            device_id={"head": other // pairs, "pair": other % pairs}, device_id_type=MESH,
        )

    def draft_outputs():
        attend(far - 1, ((G * rows, high),))
        wo_load.wait()
        r = lax.broadcasted_iota(jnp.int32, (DRAFT_ROWS, drafts), 0)
        c = lax.broadcasted_iota(jnp.int32, (DRAFT_ROWS, drafts), 1)
        for b in range(seqs):
            at_r = slice(G * rows, high)
            new = lax.dot_general(qbuf[b, at_r], dkv[0], (((1,), (1,)), ((), ())), preferred_element_type=F32)
            seen = (lax.rem(c, seqs) == b) & (c // seqs <= lax.rem(r, steps))
            new = jnp.where(seen, new, NEG)
            before = mbuf[b, at_r][:, 0:1]
            top = jnp.maximum(before, jnp.max(new, 1, keepdims=True))
            shrink = jnp.exp2((before - top) * factor)
            w = jnp.where(seen, jnp.exp2((new - top) * factor), 0.0)
            total = jnp.sum(lbuf[b, at_r], 1, keepdims=True) * shrink + jnp.sum(w, 1, keepdims=True)
            mixed = obuf[b, at_r] * shrink + jnp.dot(w.astype(BF16), dkv[1], preferred_element_type=F32)
            attn = (mixed / total).astype(BF16).astype(F32)
            aflat[b * G * steps : (b + 1) * G * steps] = attn[0 : G * steps]
        for g in range(G):
            for t in range(steps):
                lhs[t * seqs : (t + 1) * seqs, g * HEAD_DIM : (g + 1) * HEAD_DIM] = aflat[
                    pl.ds(g * steps + t, seqs, stride=G * steps), :
                ]
        partial = jnp.dot(lhs[...].astype(BF16), wo[...], preferred_element_type=F32)
        for h in range(heads):
            part[h] = partial[:, h * wide : (h + 1) * wide]
        parts[place] = part[head]

        r1 = lax.broadcasted_iota(jnp.int32, (seqs * G * steps, 1), 0)
        mine = jnp.zeros((seqs * G * steps, 1), jnp.int32)
        for p in range(seqs * G):
            mine = jnp.where(r1 // steps == p, owner_ref[0, p], mine)
        picked = jnp.where(mine == me, aflat[...], 0.0)
        found = [jnp.sum(jnp.where(lax.rem(r1, steps) == t, picked, 0.0), 0, keepdims=True) for t in range(steps)]
        dattn_ref[0, 0] = jnp.concatenate(found, 0).astype(BF16)

        for k in range(1, peers):
            give(k).start()

    def work2(s):
        pl.when(s == 1)(first_queries)
        over(LATE_B, s, functools.partial(multiply, 2))
        pl.when(s == QUERY_AT)(queries)
        pl.when(s == far)(draft_outputs)
        over(UNITS_HEAD, s, functools.partial(attend, tiles=((0, rows),)))
        over(UNITS_C, s, attend)

    ring(2, work2)

    def put(b, _):
        for g in range(G):
            at_g = slice(g * rows, (g + 1) * rows)
            total = jnp.sum(lbuf[b, at_g], 1, keepdims=True)
            ostage[g, pl.ds(b, rows, stride=seqs), :] = obuf[b, at_g] / total
        return 0

    lax.fori_loop(0, seqs, put, 0)
    for g in range(G):
        oready[:, :, g * HEAD_DIM : (g + 1) * HEAD_DIM] = ostage[g].astype(BF16).reshape(rows, seqs, HEAD_DIM)
    store = pltpu.make_async_copy(oready, out_hbm, out_sem.at[0])
    store.start()

    for k in range(1, peers):
        give(k).wait_recv()
    summed = jnp.sum(parts[...], 0)
    narrow = wide // pairs
    got = summed[:, 0:narrow]
    for j in range(1, pairs):
        got = jnp.where(pair == j, summed[:, j * narrow : (j + 1) * narrow], got)
    for t in range(steps):
        dec_ref[t] = got[t * seqs : (t + 1) * seqs].astype(BF16)

    for k in range(1, peers):
        give(k).wait_send()

    def drain(v, _):
        for k in range(len(HANDS)):
            hand(k, v).wait_send()
        return 0

    lax.fori_loop(1, shards, drain, 0)
    store.wait()


def settle(*refs):
    for k in range(3):
        refs[3 + k][...] = refs[k][...]


def body(groups, shards, heads, pairs, x, d, wq, wk, wv, wo, block_map, prompt_len, owner):
    rows, seqs, width = x.shape
    depth = wq.shape[0]
    steps = d.shape[0]
    drafts = steps * seqs
    tall = rows * seqs
    peers = heads * pairs
    high = G * rows + DRAFT_ROWS
    any_ = pl.BlockSpec(memory_space=pl.ANY)
    vmem = pl.BlockSpec(memory_space=pltpu.VMEM)
    smem = pl.BlockSpec(memory_space=pltpu.SMEM)
    dma = pltpu.SemaphoreType.DMA
    made = pl.pallas_call(
        functools.partial(kernel, groups, shards, heads, pairs),
        out_shape=(
            jax.ShapeDtypeStruct((rows, seqs, wq.shape[1]), BF16),
            jax.ShapeDtypeStruct((1, 1, steps, HEAD_DIM), BF16),
            jax.ShapeDtypeStruct((steps, seqs, wo.shape[1] // peers), BF16),
        ),
        in_specs=[any_, vmem, any_, any_, any_, any_, smem, smem, smem],
        out_specs=(any_, vmem, vmem),
        scratch_shapes=[
            pltpu.VMEM((8, shards, depth, HEAD_DIM), BF16),
            pltpu.VMEM((shards, rows, seqs, depth), BF16),
            pltpu.VMEM((shards, tall + drafts, depth), BF16),
            pltpu.VMEM((shards, drafts, depth), BF16),
            pltpu.VMEM((6, tall + drafts, HEAD_DIM), F32),
            pltpu.VMEM((seqs, high, HEAD_DIM), BF16),
            pltpu.VMEM((seqs, high, HEAD_DIM), F32),
            pltpu.VMEM((seqs, high, HEAD_DIM), F32),
            pltpu.VMEM((seqs, high, HEAD_DIM), F32),
            pltpu.VMEM((high, HEAD_DIM), jnp.int32),
            pltpu.VMEM((G, tall, HEAD_DIM), F32),
            pltpu.VMEM((rows, seqs, wq.shape[1]), BF16),
            pltpu.VMEM((rows, HEAD_DIM), F32),
            pltpu.VMEM((rows, HEAD_DIM), F32),
            pltpu.VMEM((drafts, HEAD_DIM), F32),
            pltpu.VMEM((drafts, HEAD_DIM), F32),
            pltpu.VMEM((shards, seqs, rows), jnp.int32),
            pltpu.VMEM((2, drafts, HEAD_DIM), BF16),
            pltpu.VMEM((seqs * G * steps, HEAD_DIM), F32),
            pltpu.VMEM((drafts, wq.shape[1]), F32),
            pltpu.VMEM(wo.shape, BF16),
            pltpu.VMEM((heads, drafts, wo.shape[1] // heads), F32),
            pltpu.VMEM((peers, drafts, wo.shape[1] // heads), F32),
            dma((7,)),
            dma((shards,)),
            dma((1,)),
            dma((20,)),
            dma((20, TURNS)),
            dma((len(HANDS), shards)),
            dma((len(HANDS), shards)),
            dma((2,)),
            dma((2, shards // 2)),
            dma((peers,)),
            dma((peers,)),
        ],
        compiler_params=pltpu.CompilerParams(
            collective_id=0, has_side_effects=True, vmem_limit_bytes=60 * 1024 * 1024
        ),
    )(x, d, wq, wk, wv, wo, block_map, prompt_len, owner)
    prefill, draft, decode = pl.pallas_call(
        settle,
        out_shape=tuple(jax.ShapeDtypeStruct(a.shape, a.dtype) for a in made),
        in_specs=[vmem] * 3,
        out_specs=(vmem,) * 3,
    )(*made)
    return prefill, draft.transpose(2, 0, 1, 3), decode


def solution(mesh):
    placed = (
        P("shard", "groups", None),
        P(None, "groups", "shard"),
        P("shard", ("head", "pair")),
        P("shard", ("head", "pair")),
        P("shard", ("head", "pair")),
        P(("head", "pair"), "shard"),
        P("groups"),
        P("groups"),
        P(("head", "pair"), "groups"),
    )
    sizes = [mesh.shape[name] for name in ("groups", "shard", "head", "pair")]
    return jax.shard_map(
        functools.partial(body, *sizes),
        mesh=mesh,
        in_specs=placed,
        out_specs=(
            P("shard", "groups", ("head", "pair")),
            P(None, ("groups", "shard"), ("head", "pair"), None),
            P(None, "groups", ("shard", "head", "pair")),
        ),
        check_vma=False,
    )
```

```python
import functools
import math

import jax
import jax.numpy as jnp
from jax import lax
from jax.experimental import pallas as pl
from jax.experimental.pallas import tpu as pltpu
from jax.sharding import PartitionSpec as P

HEAD_DIM = 128
G = 4
BLK = 64
NEG = -1e30
THETA = 500000.0
MESH = pl.DeviceIdType.MESH
F32 = jnp.float32
BF16 = jnp.bfloat16
FAR = 1 << 30
DRAFT_ROWS = 16

GROUPS = ((0, 1), (2, 3, 4, 5))
EXTRA = (176, 208)
PARTS = (
    ((0, 1, True), (1, 1, True), (2, 1, True), (0, 1, False), (1, 1, False)),
    ((3, 1, True), (4, 1, True), (5, 1, True), (2, 2, False), (4, 2, False)),
)
HANDS = ((0, 1, 0, 2), (0, 2, 2, 1), (1, 2, 3, 3))
NEEDS = ((0,), (1, 2))
LANES = (0, 10, 0)
TURNS = 4
UNITS_A = {2: (0, 1), 3: (1, 2), 4: (2, 3), 6: (3, 4), 7: (4, 5), 8: (5, 6)}
LATE_A = {1: (6, 7), 3: (7, 8)}
CACHE_AT = 3
UNITS_B = {4: (0, 1), 5: (1, 2), 6: (2, 3), 8: (3, 4)}
LATE_B = {1: (4, 5), 2: (5, 6), 3: (6, 7), 4: (7, 8)}
QUERY_AT = 4
UNITS_C = {4: (0, 1), 5: (1, 3), 6: (3, 5), 7: (5, 7), 8: (7, 8)}


def rope_tables(pos):
    lane = lax.broadcasted_iota(jnp.int32, (pos.shape[0], HEAD_DIM), 1)
    half = HEAD_DIM // 2
    pair = jnp.where(lane < half, lane, lane - half).astype(F32)
    freq = jnp.exp(pair * (-math.log(THETA) / half))
    angle = pos.astype(F32) * freq
    sine = jnp.sin(angle)
    return jnp.cos(angle), jnp.where(lane < half, -sine, sine)


def rope(v, cosine, sine):
    return v * cosine + pltpu.roll(v, HEAD_DIM // 2, 1) * sine


def over(table, s, f):
    low, high = jnp.int32(0), jnp.int32(0)
    for k, (a, b) in table.items():
        low = jnp.where(s == k, a, low)
        high = jnp.where(s == k, b, high)

    def one(u, _):
        f(u)
        return 0

    lax.fori_loop(low, high, one, 0)


def kernel(
    groups, shards, heads, pairs,
    x_hbm, d_ref, wq_hbm, wk_hbm, wv_hbm, wo_hbm, map_ref, len_ref, owner_ref,
    out_hbm, dattn_ref, dec_ref,
    buf, xin, xs, dbuf, acc, qbuf, mbuf, lbuf, obuf, limit, ostage, oready, cosb, sinb, dcos, dsin, kpos,
    dkv, aflat, lhs, wo, part, parts,
    load_sem, x_sem, out_sem, send_sem, recv_sem, ysend_sem, yrecv_sem, dsend_sem, drecv_sem, psend_sem, precv_sem,
):
    me = lax.axis_index("shard")
    head = lax.axis_index("head")
    pair = lax.axis_index("pair")
    group = lax.axis_index("groups")
    right = lax.rem(me + 1, shards)
    left = lax.rem(me + shards - 1, shards)
    odd = lax.rem(group, 2)
    twin = group + 1 - 2 * odd
    far = shards // 2
    rows, seqs, width = x_hbm.shape
    depth = wq_hbm.shape[0]
    steps = d_ref.shape[0]
    tall = rows * seqs
    drafts = steps * seqs
    per = rows // BLK
    scale = 1.0 / math.sqrt(HEAD_DIM)
    factor = scale * math.log2(math.e)
    peers = heads * pairs
    place = head * pairs + pair
    high = G * rows + DRAFT_ROWS

    barrier = pltpu.get_barrier_semaphore()
    for z in (left, right):
        pl.semaphore_signal(barrier, inc=1, device_id={"shard": z}, device_id_type=MESH)
    pl.semaphore_signal(barrier, inc=1, device_id={"groups": twin}, device_id_type=MESH)
    for k in range(1, peers):
        other = lax.rem(place + k, peers)
        pl.semaphore_signal(
            barrier, inc=1, device_id={"head": other // pairs, "pair": other % pairs}, device_id_type=MESH
        )

    def owner_of(v):
        half = (v + 1) // 2
        return lax.rem(me + shards + jnp.where(lax.rem(v, 2) == 1, -half, half), shards)

    sources = [wk_hbm, wv_hbm] + [wq_hbm.at[:, g * HEAD_DIM : (g + 1) * HEAD_DIM] for g in range(G)]
    loads = [pltpu.make_async_copy(src, buf.at[s, me], load_sem.at[s]) for s, src in enumerate(sources)]
    wo_load = pltpu.make_async_copy(wo_hbm, wo, load_sem.at[6])

    def x_load(owner):
        return pltpu.make_async_copy(
            x_hbm.at[:, :, pl.ds(pl.multiple_of(owner * depth, depth), depth)], xin.at[owner], x_sem.at[owner]
        )

    for load in loads:
        load.start()

    def start_x(v, _):
        x_load(owner_of(v)).start()
        return 0

    lax.fori_loop(0, shards, start_x, 0)
    wo_load.start()

    d_all = d_ref[...].astype(F32)
    dbuf[me] = jnp.concatenate([d_all[t] for t in range(steps)], 0).astype(BF16)

    pl.semaphore_wait(barrier, 2 + 1 + peers - 1)

    def pieces(phase):
        if phase == 2:
            found = [(6 + k % 2, 1, k // 2 * (depth // 2), depth // 2) for k in range(4)]
        else:
            found = []
            for stream, count, own in PARTS[phase]:
                extra = EXTRA[0 if stream in GROUPS[0] else 1]
                if own:
                    found.append((stream, count, odd * (depth - extra), extra))
                else:
                    found.append((stream, count, extra, depth - 2 * extra))
        return [(LANES[phase] + 2 * k, *piece) for k, piece in enumerate(found)]

    def hop(piece, way, s):
        lane, stream, streams, first, count = piece
        owner = lax.rem(me + shards - (s - 1), shards) if way == 0 else lax.rem(me + (s - 1), shards)
        if isinstance(s, int) and s == far:
            upper = (count // 2 + 15) // 16 * 16
            first = first + way * upper
            count = count - upper if way else upper
        if not isinstance(first, int):
            first = pl.multiple_of(first, 16)
        ref = buf.at[pl.ds(stream, streams), owner, pl.ds(first, count)]
        turn = (s - 1) % TURNS if isinstance(s, int) else lax.rem(s - 1, TURNS)
        return pltpu.make_async_remote_copy(
            src_ref=ref, dst_ref=ref, send_sem=send_sem.at[lane + way], recv_sem=recv_sem.at[lane + way, turn],
            device_id={"shard": right if way == 0 else left}, device_id_type=MESH,
        )

    def hand(k, v):
        _, _, stream, streams = HANDS[k]
        extra = EXTRA[0 if stream in GROUPS[0] else 1]
        ref = buf.at[
            pl.ds(stream, streams), owner_of(v), pl.ds(pl.multiple_of(odd * (depth - extra), 16), extra)
        ]
        return pltpu.make_async_remote_copy(
            src_ref=ref, dst_ref=ref, send_sem=ysend_sem.at[k, v], recv_sem=yrecv_sem.at[k, v],
            device_id={"groups": twin}, device_id_type=MESH,
        )

    def hands(phase, part, v):
        for k, (at, after, _, _) in enumerate(HANDS):
            if at == phase and after == part:
                hand(k, v).start()

    def draft_hop(way, s):
        owner = lax.rem(me + shards - (s - 1), shards) if way == 0 else lax.rem(me + (s - 1), shards)
        return pltpu.make_async_remote_copy(
            src_ref=dbuf.at[owner], dst_ref=dbuf.at[owner], send_sem=dsend_sem.at[way],
            recv_sem=drecv_sem.at[way, s - 1], device_id={"shard": right if way == 0 else left}, device_id_type=MESH,
        )

    def launch(phase):
        for piece in pieces(phase):
            for way in range(2):
                hop(piece, way, 1).start()
        if phase == 0:
            for way in range(2):
                draft_hop(way, 1).start()

    def pass_on(phase, s):
        for k, piece in enumerate(pieces(phase)):
            for way in range(2):
                hop(piece, way, s).wait_recv()
                hop(piece, way, s).wait_send()

                @pl.when(s < far - 1)
                def _():
                    hop(piece, way, s + 1).start()

                @pl.when(s == far - 1)
                def _():
                    hop(piece, way, far).start()

                hands(phase, k, 2 * s - 1 + way)
        if phase == 0:
            for way in range(2):
                draft_hop(way, s).wait_recv()
                draft_hop(way, s).wait_send()

            draft_hop(0, s + 1).start()

            @pl.when(s < far - 1)
            def _():
                draft_hop(1, s + 1).start()

        if phase < 2:

            @pl.when(s == far - 1)
            def _():
                launch(phase + 1)

    def finish(phase):
        for k, piece in enumerate(pieces(phase)):
            for way in range(2):
                hop(piece, way, far).wait_recv()
                hop(piece, way, far).wait_send()
            hands(phase, k, 2 * far - 1)
        if phase == 0:
            draft_hop(0, far).wait_recv()
            draft_hop(0, far).wait_send()

    def ring(phase, work):
        def step(s, _):
            @pl.when(s < far)
            def _():
                pass_on(phase, s)

            @pl.when(s == far)
            def _():
                finish(phase)

            work(s)
            return 0

        lax.fori_loop(1, far + 1, step, 0)

    def multiply(phase, u):
        streams = GROUPS[phase]

        def one(v, _):
            owner = owner_of(v)
            if phase == 0:
                x_load(owner).wait()
                xs[owner, 0:tall] = xin[owner].reshape(tall, depth)
                xs[owner, tall : tall + drafts] = dbuf[owner]

            @pl.when(v > 0)
            def _():
                for k in NEEDS[phase]:
                    hand(k, v).wait_recv()

            w = jnp.concatenate([buf[stream, owner] for stream in streams], 1)
            got = jnp.dot(xs[owner], w, preferred_element_type=F32)
            for k, stream in enumerate(streams):
                acc[stream] += got[:, k * HEAD_DIM : (k + 1) * HEAD_DIM]
            return 0

        lax.fori_loop(2 * u, 2 * u + 2, one, 0)

    def own_rows(count):
        row = lax.rem(lax.broadcasted_iota(jnp.int32, (count, 1), 0), rows)
        pos = row + map_ref[me * per] * BLK
        for j in range(1, per):
            pos = jnp.where(row >= j * BLK, row - j * BLK + map_ref[me * per + j] * BLK, pos)
        return pos

    for load in loads[:3]:
        load.wait()
    launch(0)

    for stream in range(6):
        acc[stream] = jnp.zeros(acc.shape[1:], F32)
    cosb[...], sinb[...] = rope_tables(own_rows(rows))
    drow = lax.broadcasted_iota(jnp.int32, (drafts, 1), 0)
    dpos = jnp.zeros((drafts, 1), jnp.int32)
    for t in range(steps):
        for b in range(seqs):
            dpos = jnp.where(drow == t * seqs + b, len_ref[b] + t, dpos)
    dcos[...], dsin[...] = rope_tables(dpos)
    seq = lax.broadcasted_iota(jnp.int32, (seqs, rows), 0)
    lengths = jnp.zeros((seqs, rows), jnp.int32)
    for b in range(seqs):
        lengths = jnp.where(seq == b, len_ref[b], lengths)

    def positions(z, _):
        lane = lax.broadcasted_iota(jnp.int32, (seqs, rows), 1)
        where = lane + map_ref[z * per] * BLK
        for j in range(1, per):
            where = jnp.where(lane >= j * BLK, lane - j * BLK + map_ref[z * per + j] * BLK, where)
        kpos[z] = jnp.where(where < lengths, where, FAR)
        return 0

    lax.fori_loop(0, shards, positions, 0)
    limit[0 : G * rows] = jnp.broadcast_to(own_rows(G * rows), (G * rows, HEAD_DIM))
    limit[G * rows : high] = jnp.full((DRAFT_ROWS, HEAD_DIM), FAR - 1, jnp.int32)

    for load in loads[3:]:
        load.wait()
    ring(0, lambda s: over(UNITS_A, s, functools.partial(multiply, 0)))

    def own_cache():
        def one(b, _):
            k = acc[0, pl.ds(b, rows, stride=seqs), :]
            v = acc[1, pl.ds(b, rows, stride=seqs), :]
            at = pl.ds(pl.multiple_of(b * rows, rows), rows)
            buf[6, me, at] = rope(k, cosb[...], sinb[...]).astype(BF16)
            buf[7, me, at] = v.astype(BF16)
            return 0

        lax.fori_loop(0, seqs, one, 0)
        dkv[0] = rope(acc[0, tall : tall + drafts, :], dcos[...], dsin[...]).astype(BF16)
        dkv[1] = acc[1, tall : tall + drafts, :].astype(BF16)

    def work1(s):
        over(LATE_A, s, functools.partial(multiply, 0))
        pl.when(s == CACHE_AT)(own_cache)
        over(UNITS_B, s, functools.partial(multiply, 1))

    ring(1, work1)

    def queries():
        dq = [rope(acc[2 + g, tall : tall + drafts, :], dcos[...], dsin[...]) for g in range(G)]
        for b in range(seqs):
            pieces = [dq[g][t * seqs + b : t * seqs + b + 1] for g in range(G) for t in range(steps)]
            pieces.append(jnp.zeros((DRAFT_ROWS - G * steps, HEAD_DIM), F32))
            qbuf[b, G * rows : high] = jnp.concatenate(pieces, 0).astype(BF16)

        def one(b, _):
            for g in range(G):
                q = acc[2 + g, pl.ds(b, rows, stride=seqs), :]
                qbuf[b, g * rows : (g + 1) * rows] = rope(q, cosb[...], sinb[...]).astype(BF16)
            mbuf[b] = jnp.full((high, HEAD_DIM), NEG, F32)
            lbuf[b] = jnp.zeros((high, HEAD_DIM), F32)
            obuf[b] = jnp.zeros((high, HEAD_DIM), F32)
            return 0

        lax.fori_loop(0, seqs, one, 0)

    def attend(u, tiles=((0, high),)):
        first, second = owner_of(2 * u), owner_of(2 * u + 1)

        def one(b, _):
            at = pl.ds(pl.multiple_of(b * rows, rows), rows)
            k = jnp.concatenate([buf[6, first, at, :], buf[6, second, at, :]], 0)
            v = jnp.concatenate([buf[7, first, at, :], buf[7, second, at, :]], 0)
            kp0 = kpos[first, pl.ds(b, 1), :]
            kp1 = kpos[second, pl.ds(b, 1), :]
            for low, end in tiles:
                at_r = slice(low, end)
                s = lax.dot_general(qbuf[b, at_r], k, (((1,), (1,)), ((), ())), preferred_element_type=F32)
                most = limit[at_r]
                s0 = jnp.where(kp0 <= most, s[:, 0:rows], NEG)
                s1 = jnp.where(kp1 <= most, s[:, rows : 2 * rows], NEG)
                before = mbuf[b, at_r]
                top = jnp.maximum(before, jnp.max(jnp.maximum(s0, s1), 1, keepdims=True))
                shrink = jnp.exp2((before - top) * factor)
                w0 = jnp.exp2((s0 - top) * factor)
                w1 = jnp.exp2((s1 - top) * factor)
                mbuf[b, at_r] = top
                lbuf[b, at_r] = lbuf[b, at_r] * shrink + (w0 + w1)
                w = jnp.concatenate([w0, w1], 1).astype(BF16)
                obuf[b, at_r] = obuf[b, at_r] * shrink + jnp.dot(w, v, preferred_element_type=F32)
            return 0

        lax.fori_loop(0, seqs, one, 0)

    wide = wo.shape[1] // heads

    def give(k):
        other = lax.rem(place + k, peers)
        return pltpu.make_async_remote_copy(
            src_ref=part.at[other // pairs], dst_ref=parts.at[place], send_sem=psend_sem.at[k], recv_sem=precv_sem.at[k],
            device_id={"head": other // pairs, "pair": other % pairs}, device_id_type=MESH,
        )

    def draft_outputs():
        attend(far - 1, ((G * rows, high),))
        wo_load.wait()
        r = lax.broadcasted_iota(jnp.int32, (DRAFT_ROWS, drafts), 0)
        c = lax.broadcasted_iota(jnp.int32, (DRAFT_ROWS, drafts), 1)
        for b in range(seqs):
            at_r = slice(G * rows, high)
            new = lax.dot_general(qbuf[b, at_r], dkv[0], (((1,), (1,)), ((), ())), preferred_element_type=F32)
            seen = (lax.rem(c, seqs) == b) & (c // seqs <= lax.rem(r, steps))
            new = jnp.where(seen, new, NEG)
            before = mbuf[b, at_r][:, 0:1]
            top = jnp.maximum(before, jnp.max(new, 1, keepdims=True))
            shrink = jnp.exp2((before - top) * factor)
            w = jnp.where(seen, jnp.exp2((new - top) * factor), 0.0)
            total = jnp.sum(lbuf[b, at_r], 1, keepdims=True) * shrink + jnp.sum(w, 1, keepdims=True)
            mixed = obuf[b, at_r] * shrink + jnp.dot(w.astype(BF16), dkv[1], preferred_element_type=F32)
            attn = (mixed / total).astype(BF16).astype(F32)
            aflat[b * G * steps : (b + 1) * G * steps] = attn[0 : G * steps]
        for g in range(G):
            for t in range(steps):
                lhs[t * seqs : (t + 1) * seqs, g * HEAD_DIM : (g + 1) * HEAD_DIM] = aflat[
                    pl.ds(g * steps + t, seqs, stride=G * steps), :
                ]
        partial = jnp.dot(lhs[...].astype(BF16), wo[...], preferred_element_type=F32)
        for h in range(heads):
            part[h] = partial[:, h * wide : (h + 1) * wide]
        parts[place] = part[head]

        r1 = lax.broadcasted_iota(jnp.int32, (seqs * G * steps, 1), 0)
        mine = jnp.zeros((seqs * G * steps, 1), jnp.int32)
        for p in range(seqs * G):
            mine = jnp.where(r1 // steps == p, owner_ref[0, p], mine)
        picked = jnp.where(mine == me, aflat[...], 0.0)
        found = [jnp.sum(jnp.where(lax.rem(r1, steps) == t, picked, 0.0), 0, keepdims=True) for t in range(steps)]
        dattn_ref[0, 0] = jnp.concatenate(found, 0).astype(BF16)

        for k in range(1, peers):
            give(k).start()

    def work2(s):
        over(LATE_B, s, functools.partial(multiply, 1))
        pl.when(s == QUERY_AT)(queries)
        pl.when(s == far)(draft_outputs)
        over(UNITS_C, s, attend)

    ring(2, work2)

    def put(b, _):
        for g in range(G):
            at_g = slice(g * rows, (g + 1) * rows)
            total = jnp.sum(lbuf[b, at_g], 1, keepdims=True)
            ostage[g, pl.ds(b, rows, stride=seqs), :] = obuf[b, at_g] / total
        return 0

    lax.fori_loop(0, seqs, put, 0)
    for g in range(G):
        oready[:, :, g * HEAD_DIM : (g + 1) * HEAD_DIM] = ostage[g].astype(BF16).reshape(rows, seqs, HEAD_DIM)
    store = pltpu.make_async_copy(oready, out_hbm, out_sem.at[0])
    store.start()

    for k in range(1, peers):
        give(k).wait_recv()
    summed = jnp.sum(parts[...], 0)
    narrow = wide // pairs
    got = summed[:, 0:narrow]
    for j in range(1, pairs):
        got = jnp.where(pair == j, summed[:, j * narrow : (j + 1) * narrow], got)
    for t in range(steps):
        dec_ref[t] = got[t * seqs : (t + 1) * seqs].astype(BF16)

    for k in range(1, peers):
        give(k).wait_send()

    def drain(v, _):
        for k in range(len(HANDS)):
            hand(k, v).wait_send()
        return 0

    lax.fori_loop(1, shards, drain, 0)
    store.wait()


def settle(*refs):
    for k in range(3):
        refs[3 + k][...] = refs[k][...]


def body(groups, shards, heads, pairs, x, d, wq, wk, wv, wo, block_map, prompt_len, owner):
    rows, seqs, width = x.shape
    depth = wq.shape[0]
    steps = d.shape[0]
    drafts = steps * seqs
    tall = rows * seqs
    peers = heads * pairs
    high = G * rows + DRAFT_ROWS
    any_ = pl.BlockSpec(memory_space=pl.ANY)
    vmem = pl.BlockSpec(memory_space=pltpu.VMEM)
    smem = pl.BlockSpec(memory_space=pltpu.SMEM)
    dma = pltpu.SemaphoreType.DMA
    made = pl.pallas_call(
        functools.partial(kernel, groups, shards, heads, pairs),
        out_shape=(
            jax.ShapeDtypeStruct((rows, seqs, wq.shape[1]), BF16),
            jax.ShapeDtypeStruct((1, 1, steps, HEAD_DIM), BF16),
            jax.ShapeDtypeStruct((steps, seqs, wo.shape[1] // peers), BF16),
        ),
        in_specs=[any_, vmem, any_, any_, any_, any_, smem, smem, smem],
        out_specs=(any_, vmem, vmem),
        scratch_shapes=[
            pltpu.VMEM((8, shards, depth, HEAD_DIM), BF16),
            pltpu.VMEM((shards, rows, seqs, depth), BF16),
            pltpu.VMEM((shards, tall + drafts, depth), BF16),
            pltpu.VMEM((shards, drafts, depth), BF16),
            pltpu.VMEM((6, tall + drafts, HEAD_DIM), F32),
            pltpu.VMEM((seqs, high, HEAD_DIM), BF16),
            pltpu.VMEM((seqs, high, HEAD_DIM), F32),
            pltpu.VMEM((seqs, high, HEAD_DIM), F32),
            pltpu.VMEM((seqs, high, HEAD_DIM), F32),
            pltpu.VMEM((high, HEAD_DIM), jnp.int32),
            pltpu.VMEM((G, tall, HEAD_DIM), F32),
            pltpu.VMEM((rows, seqs, wq.shape[1]), BF16),
            pltpu.VMEM((rows, HEAD_DIM), F32),
            pltpu.VMEM((rows, HEAD_DIM), F32),
            pltpu.VMEM((drafts, HEAD_DIM), F32),
            pltpu.VMEM((drafts, HEAD_DIM), F32),
            pltpu.VMEM((shards, seqs, rows), jnp.int32),
            pltpu.VMEM((2, drafts, HEAD_DIM), BF16),
            pltpu.VMEM((seqs * G * steps, HEAD_DIM), F32),
            pltpu.VMEM((drafts, wq.shape[1]), F32),
            pltpu.VMEM(wo.shape, BF16),
            pltpu.VMEM((heads, drafts, wo.shape[1] // heads), F32),
            pltpu.VMEM((peers, drafts, wo.shape[1] // heads), F32),
            dma((7,)),
            dma((shards,)),
            dma((1,)),
            dma((20,)),
            dma((20, TURNS)),
            dma((len(HANDS), shards)),
            dma((len(HANDS), shards)),
            dma((2,)),
            dma((2, shards // 2)),
            dma((peers,)),
            dma((peers,)),
        ],
        compiler_params=pltpu.CompilerParams(
            collective_id=0, has_side_effects=True, vmem_limit_bytes=60 * 1024 * 1024
        ),
    )(x, d, wq, wk, wv, wo, block_map, prompt_len, owner)
    prefill, draft, decode = pl.pallas_call(
        settle,
        out_shape=tuple(jax.ShapeDtypeStruct(a.shape, a.dtype) for a in made),
        in_specs=[vmem] * 3,
        out_specs=(vmem,) * 3,
    )(*made)
    return prefill, draft.transpose(2, 0, 1, 3), decode


def solution(mesh):
    placed = (
        P("shard", "groups", None),
        P(None, "groups", "shard"),
        P("shard", ("head", "pair")),
        P("shard", ("head", "pair")),
        P("shard", ("head", "pair")),
        P(("head", "pair"), "shard"),
        P("groups"),
        P("groups"),
        P(("head", "pair"), "groups"),
    )
    sizes = [mesh.shape[name] for name in ("groups", "shard", "head", "pair")]
    return jax.shard_map(
        functools.partial(body, *sizes),
        mesh=mesh,
        in_specs=placed,
        out_specs=(
            P("shard", "groups", ("head", "pair")),
            P(None, ("groups", "shard"), ("head", "pair"), None),
            P(None, "groups", ("shard", "head", "pair")),
        ),
        check_vma=False,
    )
```
